32 devices in a mesh: bias: 2 (over x), ea: 16 (over z, y, core).
Axes of the slice: x: 2, y: 2, z: 4, core: 2. Of those that a mesh axis runs over, the one named last changes fastest.
Arguments:
- g_lesser: bfloat16 [512, 2, 256, 256], P(('bias', 'ea')), parts along dimension 0, may hold values from -6 to 6
- g_greater: bfloat16 [512, 2, 256, 256], P(('bias', 'ea')), parts along dimension 0, may hold values from -6 to 6
- g_free: bfloat16 [512, 2, 256, 256], P(('bias', 'ea')), parts along dimension 0, may hold values from -3 to 3
- coulomb: bfloat16 [256, 256], replicated, may hold values from -0.375 to 0.375
Outputs:
- g_new: bfloat16 [512, 2, 256, 256], P(('bias', 'ea')), parts along dimension 0
The draws below stay inside these ranges and needn't reach their ends.
There are 2 independent parts, one for each index of `bias`. The reference program is written for one: setup_inputs(seed, part) draws one part's arguments, and reference() takes and returns one part's arrays. A program takes and returns all parts, laid end to end along the dimension named above; an argument that names none is the same for every part. Nothing has to cross between parts.
All inputs are finite; a program needn't handle non-finite values.
Results may differ from the reference program's by a relative error of at most 0.022.
Values may be sent and summed in bfloat16 or wider, within the bound.
A program may use at most 192 MiB of HBM per device.

```python
import jax
import jax.numpy as jnp

NO = 256
NE = 256


def levels(rng, extent, shards, least, top_value):
    def one(position, parts):
        steps = jax.random.uniform(jax.random.fold_in(jax.random.fold_in(rng, 6), position), (parts,), jnp.float32, least / len(shards), top_value / len(shards))
        return jnp.repeat(jnp.exp(steps), extent[position] // parts).reshape((-1,) + (1,) * (len(extent) - position - 1))

    gain = one(*shards[0])
    for cut in shards[1:]:
        gain = gain * one(*cut)
    return gain


def gaussian(own_key, shape, width, reach, split=(), held_as=jnp.bfloat16):
    level = levels(own_key, shape, split, -0.22, 0.18) if split else 1.0
    entries = jax.random.normal(own_key, shape, jnp.float32) * width * level
    return jnp.minimum(jnp.maximum(entries, -reach), reach).astype(held_as)


def setup_inputs(seed: int = 0, part: int = 0) -> dict:
    key_list = jax.random.split(jax.random.key(seed), 5)
    part_keys = jax.random.split(jax.random.fold_in(key_list[4], part), 5)
    g_lesser = gaussian(part_keys[0], (NE, 2, NO, NO), 1.0, 6.0, ((0, 16),))
    g_greater = gaussian(part_keys[1], (NE, 2, NO, NO), 1.0, 6.0, ((0, 16),))
    g_free = gaussian(part_keys[2], (NE, 2, NO, NO), 0.5, 3.0, ((0, 16),))
    coulomb = gaussian(key_list[3], (NO, NO), NO ** -0.5, 0.375)
    return dict(g_lesser=g_lesser, g_greater=g_greater, g_free=g_free, coulomb=coulomb)


def as_complex(block):
    return block[:, 0].astype(jnp.float32) + 1j * block[:, 1].astype(jnp.float32)


def batched(left, right):
    return jnp.einsum("eij,ejk->eik", left.astype(jnp.float32), right.astype(jnp.float32))


def reference(g_lesser, g_greater, g_free, coulomb):
    length = 2 * NE
    lesser = as_complex(g_lesser)
    greater_t = jnp.swapaxes(as_complex(g_greater), 1, 2)
    spec_lesser = jnp.fft.fft(lesser, n=length, axis=0)
    spec_greater = jnp.fft.ifft(greater_t, n=length, axis=0) * length
    polar = jnp.fft.ifft(spec_lesser * spec_greater, axis=0)[:NE] / NE
    polar_real = polar.real.astype(jnp.bfloat16)
    polar_imag = polar.imag.astype(jnp.bfloat16)
    volts = coulomb.astype(jnp.float32)
    mixed_real = jnp.einsum("eij,jk->eik", polar_real.astype(jnp.float32), volts).astype(jnp.bfloat16)
    mixed_imag = jnp.einsum("eij,jk->eik", polar_imag.astype(jnp.float32), volts).astype(jnp.bfloat16)
    square_real = batched(mixed_real, mixed_real) - batched(mixed_imag, mixed_imag)
    square_imag = batched(mixed_real, mixed_imag) + batched(mixed_imag, mixed_real)
    inner_real = (mixed_real.astype(jnp.float32) + square_real).astype(jnp.bfloat16)
    inner_imag = (mixed_imag.astype(jnp.float32) + square_imag).astype(jnp.bfloat16)
    screen_real = (volts[None] + jnp.einsum("ij,ejk->eik", volts, inner_real.astype(jnp.float32))).astype(jnp.bfloat16)
    screen_imag = jnp.einsum("ij,ejk->eik", volts, inner_imag.astype(jnp.float32)).astype(jnp.bfloat16)
    screen = screen_real.astype(jnp.float32) + 1j * screen_imag.astype(jnp.float32)
    spec_screen = jnp.fft.fft(screen, n=length, axis=0)
    sigma = jnp.fft.ifft(spec_lesser * spec_screen, axis=0)[:NE] / NE
    sigma_real = sigma.real.astype(jnp.bfloat16)
    sigma_imag = sigma.imag.astype(jnp.bfloat16)
    free_real = g_free[:, 0]
    free_imag = g_free[:, 1]
    right_real = (batched(sigma_real, free_real) - batched(sigma_imag, free_imag)).astype(jnp.bfloat16)
    right_imag = (batched(sigma_real, free_imag) + batched(sigma_imag, free_real)).astype(jnp.bfloat16)
    out_real = free_real.astype(jnp.float32) + batched(free_real, right_real) - batched(free_imag, right_imag)
    out_imag = free_imag.astype(jnp.float32) + batched(free_real, right_imag) + batched(free_imag, right_real)
    return jnp.stack([out_real, out_imag], axis=1).astype(jnp.bfloat16)
```

```python
import functools
import math

import jax
import jax.numpy as jnp
import numpy as np
from jax import lax
from jax.experimental import pallas as pl
from jax.experimental.pallas import tpu as pltpu
from jax.sharding import PartitionSpec as P

NE = 256


def dft_tables(length, count):
    freq = jnp.arange(length, dtype=jnp.int32)
    places = jnp.arange(count, dtype=jnp.int32)
    phase = freq[:, None] * places[None, :] % length
    angle = phase.astype(jnp.float32) * (2.0 * math.pi / length)
    cosine = jnp.cos(angle)
    sine = jnp.sin(angle)
    stacked = jnp.concatenate([cosine, sine], axis=0)
    upper = stacked.astype(jnp.bfloat16)
    lower = (stacked - upper.astype(jnp.float32)).astype(jnp.bfloat16)
    backward = jnp.concatenate([cosine.T, sine.T], axis=0)
    return (upper, lower, backward)


def forward(tables, block, sign):
    upper, lower = tables
    length = upper.shape[0] // 2
    real_part = block[:, 0].reshape(block.shape[0], -1)
    imag_part = block[:, 1].reshape(block.shape[0], -1)
    width = real_part.shape[1]
    joined = jnp.concatenate([real_part, imag_part], axis=1)
    result = jnp.dot(upper, joined, preferred_element_type=jnp.float32)
    result = result + jnp.dot(lower, joined, preferred_element_type=jnp.float32)
    cos_real = result[:length, :width]
    cos_imag = result[:length, width:]
    sin_real = result[length:, :width]
    sin_imag = result[length:, width:]
    return (cos_real - sign * sin_imag, cos_imag + sign * sin_real)


def inverse(backward, real_part, imag_part, scale):
    count = backward.shape[0] // 2
    width = real_part.shape[1]
    joined = jnp.concatenate([real_part, imag_part], axis=1)
    result = jnp.dot(
        backward, joined, precision=lax.Precision.HIGH, preferred_element_type=jnp.float32
    )
    cos_real = result[:count, :width]
    cos_imag = result[:count, width:]
    sin_real = result[count:, :width]
    sin_imag = result[count:, width:]
    return ((cos_real - sin_imag) * scale, (cos_imag + sin_real) * scale)


def complex_mul(left, right):
    return (left[0] * right[0] - left[1] * right[1], left[0] * right[1] + left[1] * right[0])


def restack(real_part, imag_part, shape):
    return jnp.stack([real_part.reshape(shape), imag_part.reshape(shape)], axis=1).astype(
        jnp.bfloat16
    )


def batched(left, right):
    return jnp.einsum("eij,ejk->eik", left, right, preferred_element_type=jnp.float32)


def dyson(sigma_real, sigma_imag, g_free):
    free_real = g_free[:, 0]
    free_imag = g_free[:, 1]
    right_real = (batched(sigma_real, free_real) - batched(sigma_imag, free_imag)).astype(
        jnp.bfloat16
    )
    right_imag = (batched(sigma_real, free_imag) + batched(sigma_imag, free_real)).astype(
        jnp.bfloat16
    )
    out_real = (
        free_real.astype(jnp.float32)
        + batched(free_real, right_real)
        - batched(free_imag, right_imag)
    )
    out_imag = (
        free_imag.astype(jnp.float32)
        + batched(free_real, right_imag)
        + batched(free_imag, right_real)
    )
    return jnp.stack([out_real, out_imag], axis=1).astype(jnp.bfloat16)


def plain(g_lesser, g_greater, g_free, coulomb):
    length = 2 * NE
    upper, lower, backward = dft_tables(length, NE)
    tables = (upper, lower)
    scale = 1.0 / (length * NE)
    greater_t = jnp.swapaxes(g_greater, 2, 3)
    lesser_rows, greater_rows = (
        lax.all_to_all(g_lesser, "ea", split_axis=2, concat_axis=0, tiled=True),
        lax.all_to_all(greater_t, "ea", split_axis=2, concat_axis=0, tiled=True),
    )
    spec_lesser = forward(tables, lesser_rows, -1.0)
    element_shape = (NE, lesser_rows.shape[2], lesser_rows.shape[3])
    spec_greater = forward(tables, greater_rows, 1.0)
    joined = complex_mul(spec_lesser, spec_greater)
    polar_real, polar_imag = inverse(backward, joined[0], joined[1], scale)
    polar_rows = restack(polar_real, polar_imag, element_shape)
    polar = lax.all_to_all(polar_rows, "ea", split_axis=0, concat_axis=2, tiled=True)
    mixed_real = jnp.einsum(
        "eij,jk->eik", polar[:, 0], coulomb, preferred_element_type=jnp.float32
    ).astype(jnp.bfloat16)
    mixed_imag = jnp.einsum(
        "eij,jk->eik", polar[:, 1], coulomb, preferred_element_type=jnp.float32
    ).astype(jnp.bfloat16)
    square_real = batched(mixed_real, mixed_real) - batched(mixed_imag, mixed_imag)
    square_imag = batched(mixed_real, mixed_imag) + batched(mixed_imag, mixed_real)
    inner_real = (mixed_real.astype(jnp.float32) + square_real).astype(jnp.bfloat16)
    inner_imag = (mixed_imag.astype(jnp.float32) + square_imag).astype(jnp.bfloat16)
    screen_real = coulomb.astype(jnp.float32)[None] + jnp.einsum(
        "ij,ejk->eik", coulomb, inner_real, preferred_element_type=jnp.float32
    )
    screen_imag = jnp.einsum("ij,ejk->eik", coulomb, inner_imag, preferred_element_type=jnp.float32)
    screen = jnp.stack([screen_real, screen_imag], axis=1).astype(jnp.bfloat16)
    screen_rows = lax.all_to_all(screen, "ea", split_axis=2, concat_axis=0, tiled=True)
    spec_screen = forward(tables, screen_rows, -1.0)
    folded = complex_mul(spec_lesser, spec_screen)
    sigma_real, sigma_imag = inverse(backward, folded[0], folded[1], scale)
    sigma_rows = restack(sigma_real, sigma_imag, element_shape)
    sigma = lax.all_to_all(sigma_rows, "ea", split_axis=0, concat_axis=2, tiled=True)
    return dyson(sigma[:, 0], sigma[:, 1], g_free)


MESH = pl.DeviceIdType.MESH
CHUNKS = 4
LANES = 128
VMEM_BYTES = 60 * 1024 * 1024


def transform_table(count):
    length = 2 * count
    phase = np.arange(length)[:, None] * np.arange(count)[None, :] % length
    angle = phase * (2.0 * math.pi / length)
    cosine, sine = np.cos(angle), np.sin(angle)
    return np.block([[cosine, sine], [-sine, cosine]]).astype(np.float32)


class Place:
    def __init__(self, n):
        self.n = n
        self.side = n // 2
        self.plane = lax.axis_index("bias")
        self.me = lax.axis_index("ea")
        self.half = lax.div(self.me, self.side)
        self.seat = lax.rem(self.me, self.side)
        self.member = self.plane * self.side + self.seat

    def of_member(self, member):
        return {
            "bias": lax.div(member, self.side),
            "ea": self.half * self.side + lax.rem(member, self.side),
        }


def greet(place):
    n = place.n
    barrier = pltpu.get_barrier_semaphore()
    mine = place.plane * n + place.me

    def hello(k, carry):
        other = lax.rem(mine + k, 2 * n)
        pl.semaphore_signal(
            barrier,
            inc=1,
            device_id={"bias": lax.div(other, n), "ea": lax.rem(other, n)},
            device_id_type=MESH,
        )
        return carry

    lax.fori_loop(1, 2 * n, hello, 0)
    pl.semaphore_wait(barrier, 2 * n - 1)


def loop(low, high, body):
    def step(k, carry):
        body(k)
        return carry

    lax.fori_loop(low, high, step, 0)


def fold_row(first, scale, count, table, table_t, lesser_buf, other_buf, folded, volts, row):
    length = 2 * count
    left = jnp.concatenate([lesser_buf[0, row], lesser_buf[1, row]], axis=0)
    imag = other_buf[1, row]
    right = jnp.concatenate([other_buf[0, row], -imag if first else imag], axis=0)
    left_spec = jnp.dot(table[...], left, preferred_element_type=jnp.float32)
    right_spec = jnp.dot(table[...], right, preferred_element_type=jnp.float32)
    left_real, left_imag = left_spec[:length], left_spec[length:]
    right_real, right_imag = right_spec[:length], right_spec[length:]
    if first:
        real = left_real * right_real + left_imag * right_imag
        imag = left_imag * right_real - left_real * right_imag
    else:
        real = left_real * right_real - left_imag * right_imag
        imag = left_real * right_imag + left_imag * right_real
    product = jnp.concatenate([real, imag], axis=0).astype(jnp.bfloat16)
    result = jnp.dot(table_t[...], product, preferred_element_type=jnp.float32) * scale
    result = result.astype(jnp.bfloat16)
    if first:
        result = jnp.dot(result, volts[...], preferred_element_type=jnp.float32)
        result = result.astype(jnp.bfloat16)
    folded[0, row] = result[:count]
    folded[1, row] = result[count:]


def polarize_kernel(
    n, count, scale, lesser, other, table, table_t, volts, out, kept,
    lesser_buf, other_buf, folded, in_send, in_recv, out_send, out_recv, own_in, own_out, keep,
    swap_send, swap_recv, lesser_raw, other_raw, lesser_rows, other_rows,
):
    place = Place(n)
    me, plane, half, side = place.me, place.plane, place.half, place.side
    rows = folded.shape[1]
    each = count // n
    group = rows // CHUNKS
    wide = side * group
    stages = (lesser_rows, other_rows)
    targets = (lesser_buf, other_buf)

    def swap(s, q):
        span = pl.ds(q * wide, wide)
        return pltpu.make_async_remote_copy(
            src_ref=stages[s].at[2, :, span],
            dst_ref=stages[s].at[plane, :, span],
            send_sem=swap_send.at[s, q],
            recv_sem=swap_recv.at[s, q],
            device_id={"bias": 1 - plane},
            device_id_type=MESH,
        )

    def ends(s, q, peer):
        source = stages[s].at[
            lax.div(peer, side), :, pl.ds(q * wide + lax.rem(peer, side) * group, group)
        ]
        target = targets[s].at[:, pl.ds(q * group, group), pl.ds(me * each, each)]
        return source, target

    def incoming(s, q, k):
        peer = lax.rem(me + k, n)
        source, target = ends(s, q, peer)
        return pltpu.make_async_remote_copy(
            src_ref=source,
            dst_ref=target,
            send_sem=in_send.at[s, q, k],
            recv_sem=in_recv.at[s, q, k],
            device_id={"ea": peer},
            device_id_type=MESH,
        )

    def own_incoming(s, q):
        source, target = ends(s, q, me)
        return pltpu.make_async_copy(source, target, own_in.at[s, q])

    def spread(s, q, bias):
        def send_one(j):
            peer = bias * side + lax.rem(place.seat + j, side)
            k = lax.rem(peer - me + n, n)

            @pl.when(k == 0)
            def _():
                own_incoming(s, q).start()

            @pl.when(k != 0)
            def _():
                incoming(s, q, k).start()

        loop(0, side, send_one)

    def outgoing(q, k):
        peer = lax.rem(place.member + k, n)
        return pltpu.make_async_remote_copy(
            src_ref=folded.at[:, pl.ds(q * group, group), pl.ds(peer * each, each)],
            dst_ref=out.at[:, pl.ds((q * n + place.member) * group, group)],
            send_sem=out_send.at[q, k],
            recv_sem=out_recv.at[q, k],
            device_id=place.of_member(peer),
            device_id_type=MESH,
        )

    def own_outgoing(q):
        return pltpu.make_async_copy(
            folded.at[:, pl.ds(q * group, group), pl.ds(place.member * each, each)],
            out.at[:, pl.ds((q * n + place.member) * group, group)],
            own_out.at[q],
        )

    raw = (
        pltpu.make_async_copy(lesser, lesser_raw, keep.at[0]),
        pltpu.make_async_copy(other, other_raw, keep.at[1]),
    )
    for copy in raw:
        copy.start()
    greet(place)
    raw[0].wait()

    def regroup(q):
        for h in range(2):
            slot = jnp.where(plane == h, h, 2)
            block = pl.ds(pl.multiple_of((2 * q + h) * wide, wide), wide)
            for c in range(2):
                lesser_rows[slot, c, pl.ds(pl.multiple_of(q * wide, wide), wide)] = jnp.swapaxes(
                    lesser_raw[:, c, block, :], 0, 1
                )
        swap(0, q).start()
        spread(0, q, plane)

    loop(0, CHUNKS, regroup)
    raw[1].wait()
    for low in range(0, rows * n, LANES):
        for c in range(2):
            turned = jnp.stack(
                [other_raw[e, c, :, low : low + LANES].T for e in range(each)], axis=0
            )
            turned = jnp.swapaxes(turned, 0, 1)
            for at in range(0, LANES, wide):
                piece = (low + at) // wide
                slot = jnp.where(plane == piece % 2, piece % 2, 2)
                start = piece // 2 * wide
                other_rows[slot, c, start : start + wide] = turned[at : at + wide]
    loop(0, CHUNKS, lambda q: swap(1, q).start())

    def relay(q):
        swap(0, q).wait_recv()
        spread(0, q, 1 - plane)

    loop(0, CHUNKS, relay)

    def relay_other(q):
        spread(1, q, plane)
        swap(1, q).wait_recv()
        spread(1, q, 1 - plane)

    loop(0, CHUNKS, relay_other)

    def work(q):
        for s in range(2):
            loop(1, n, lambda k: incoming(s, q, k).wait_recv())
            own_incoming(s, q).wait()
        loop(
            q * group,
            (q + 1) * group,
            functools.partial(
                fold_row, True, scale, count, table, table_t, lesser_buf, other_buf, folded, volts
            ),
        )
        loop(1, n, lambda k: outgoing(q, k).start())
        own_outgoing(q).start()

    loop(0, CHUNKS, work)
    keeping = pltpu.make_async_copy(lesser_buf, kept, keep.at[0])
    keeping.start()

    def finish(q):
        for s in range(2):
            swap(s, q).wait_send()
            loop(1, n, lambda k: incoming(s, q, k).wait_send())
        loop(1, n, lambda k: outgoing(q, k).wait())
        own_outgoing(q).wait()

    loop(0, CHUNKS, finish)
    keeping.wait()


def dress_kernel(
    n, count, scale, kept, screen, table, table_t, out,
    lesser_buf, other_buf, folded, in_send, in_recv, out_send, out_recv, own_in, own_out, keep,
):
    place = Place(n)
    me, plane, half = place.me, place.plane, place.half
    rows = folded.shape[1]
    each = count // n
    group = rows // CHUNKS

    def incoming(q, k):
        peer = lax.rem(place.member + k, n)
        return pltpu.make_async_remote_copy(
            src_ref=screen.at[:, pl.ds((q * n + peer) * group, group)],
            dst_ref=other_buf.at[:, pl.ds(q * group, group), pl.ds(place.member * each, each)],
            send_sem=in_send.at[q, k],
            recv_sem=in_recv.at[q, k],
            device_id=place.of_member(peer),
            device_id_type=MESH,
        )

    def own_incoming(q):
        return pltpu.make_async_copy(
            screen.at[:, pl.ds((q * n + place.member) * group, group)],
            other_buf.at[:, pl.ds(q * group, group), pl.ds(place.member * each, each)],
            own_in.at[q],
        )

    def outgoing(q, k, sender):
        peer = lax.rem(me + k, n)
        return pltpu.make_async_remote_copy(
            src_ref=folded.at[:, pl.ds(q * group, group), pl.ds(peer * each, each)],
            dst_ref=out.at[:, pl.ds((q * n + place.member) * group, group)],
            send_sem=out_send.at[q, k],
            recv_sem=out_recv.at[q, sender],
            device_id={"bias": half, "ea": peer},
            device_id_type=MESH,
        )

    def own_outgoing(q):
        return pltpu.make_async_copy(
            folded.at[:, pl.ds(q * group, group), pl.ds(me * each, each)],
            out.at[:, pl.ds((q * n + place.member) * group, group)],
            own_out.at[q],
        )

    at_home = plane == half
    keeping = pltpu.make_async_copy(kept, lesser_buf, keep.at[0])
    keeping.start()
    loop(0, CHUNKS, lambda q: own_incoming(q).start())
    greet(place)
    loop(0, CHUNKS, lambda q: loop(1, n, lambda k: incoming(q, k).start()))
    keeping.wait()

    def work(q):
        loop(1, n, lambda k: incoming(q, k).wait_recv())
        own_incoming(q).wait()
        loop(
            q * group,
            (q + 1) * group,
            functools.partial(
                fold_row, False, scale, count, table, table_t, lesser_buf, other_buf, folded, None
            ),
        )

        @pl.when(at_home)
        def _():
            own_outgoing(q).start()

        @pl.when(jnp.logical_not(at_home))
        def _():
            outgoing(q, 0, place.member).start()

        loop(1, n, lambda k: outgoing(q, k, place.member).start())

    loop(0, CHUNKS, work)

    def finish(q):
        loop(1, n, lambda k: incoming(q, k).wait_send())
        loop(1, n, lambda k: outgoing(q, k, place.member).wait_send())

        @pl.when(at_home)
        def _():
            own_outgoing(q).wait()

        @pl.when(jnp.logical_not(at_home))
        def _():
            outgoing(q, 0, place.member).wait_send()

        def wait_one(sender):
            @pl.when(jnp.logical_not(jnp.logical_and(at_home, sender == place.member)))
            def _():
                outgoing(q, 0, sender).wait_recv()

        loop(0, n, wait_one)

    loop(0, CHUNKS, finish)


def exchange(n, count, first, scale, operands):
    orbitals, width = operands[1].shape[-3 if not first else -2], operands[1].shape[-1]
    each = count // n
    rows = orbitals // n
    hbm = pl.BlockSpec(memory_space=pl.ANY)
    vmem = pl.BlockSpec(memory_space=pltpu.VMEM)
    out_shape = [jax.ShapeDtypeStruct((2, orbitals, each, width), jnp.bfloat16)]
    if first:
        out_shape.append(jax.ShapeDtypeStruct((2, rows, count, width), jnp.bfloat16))
    buffer = pltpu.VMEM((2, rows, count, width), jnp.bfloat16)
    dma = pltpu.SemaphoreType.DMA
    lead = (2, CHUNKS) if first else (CHUNKS,)
    scratch = [
        buffer, buffer, buffer,
        dma(lead + (n,)), dma(lead + (n,)), dma((CHUNKS, n)), dma((CHUNKS, n)),
        dma(lead), dma((CHUNKS,)), dma((2,)),
    ]
    if first:
        scratch += [dma((2, CHUNKS))] * 2
        scratch += [pltpu.VMEM((each, 2, orbitals, width), jnp.bfloat16)] * 2
        scratch += [pltpu.VMEM((3, 2, orbitals // 2, each, width), jnp.bfloat16)] * 2
    return pl.pallas_call(
        functools.partial(polarize_kernel if first else dress_kernel, n, count, scale),
        name="polarize" if first else "dress",
        out_shape=out_shape,
        in_specs=[hbm, hbm] + [vmem] * (len(operands) - 2),
        out_specs=[hbm] * len(out_shape),
        scratch_shapes=scratch,
        compiler_params=pltpu.CompilerParams(
            collective_id=0 if first else 1, has_side_effects=True, vmem_limit_bytes=VMEM_BYTES
        ),
    )(*operands)


def dot(left, right):
    return jnp.dot(left, right, preferred_element_type=jnp.float32)


def screen_kernel(mixed, volts, out):
    bare = volts[...]
    for e in range(mixed.shape[0]):
        real, imag = mixed[e, 0], mixed[e, 1]
        square_real = dot(real, real) - dot(imag, imag)
        square_imag = dot(real, imag) + dot(imag, real)
        inner_real = (real.astype(jnp.float32) + square_real).astype(jnp.bfloat16)
        inner_imag = (imag.astype(jnp.float32) + square_imag).astype(jnp.bfloat16)
        out[e, 0] = (bare.astype(jnp.float32) + dot(bare, inner_real)).astype(jnp.bfloat16)
        out[e, 1] = dot(bare, inner_imag).astype(jnp.bfloat16)


def dyson_kernel(sigma, free, out):
    for e in range(sigma.shape[0]):
        real, imag = sigma[e, 0], sigma[e, 1]
        free_real, free_imag = free[e, 0], free[e, 1]
        right_real = (dot(real, free_real) - dot(imag, free_imag)).astype(jnp.bfloat16)
        right_imag = (dot(real, free_imag) + dot(imag, free_real)).astype(jnp.bfloat16)
        out_real = dot(free_real, right_real) - dot(free_imag, right_imag)
        out_imag = dot(free_real, right_imag) + dot(free_imag, right_real)
        out[e, 0] = (free_real.astype(jnp.float32) + out_real).astype(jnp.bfloat16)
        out[e, 1] = (free_imag.astype(jnp.float32) + out_imag).astype(jnp.bfloat16)


def per_energy(kernel, name, matrices, others):
    each, two, rows, width = matrices.shape
    block = pl.BlockSpec((2, two, rows, width), lambda i: (i, 0, 0, 0))
    specs = [block if other.ndim == 4 else pl.BlockSpec(memory_space=pltpu.VMEM) for other in others]
    products = 6 if name == "screen" else 8
    return pl.pallas_call(
        kernel,
        name=name,
        grid=(each // 2,),
        out_shape=jax.ShapeDtypeStruct(matrices.shape, jnp.bfloat16),
        in_specs=[block] + specs,
        out_specs=block,
        cost_estimate=pl.CostEstimate(
            flops=2 * products * each * rows * rows * width,
            bytes_accessed=4 * two * each * rows * width,
            transcendentals=0,
        ),
    )(matrices, *others)


def per_device(n, biases, g_lesser, g_greater, g_free, coulomb):
    each, _, orbitals, _ = g_lesser.shape
    count = n * each
    if biases != 2 or n % 2 or each % 16 or orbitals % (n * 16) or LANES % (n // 2 * orbitals // n // CHUNKS):
        return plain(g_lesser, g_greater, g_free, coulomb)
    scale = 1.0 / (2 * count * count)
    full = transform_table(count)
    table = jnp.asarray(full).astype(jnp.bfloat16)
    table_t = jnp.asarray(full.T).astype(jnp.bfloat16)
    mixed, kept = exchange(n, count, True, scale, (g_lesser, g_greater, table, table_t, coulomb))
    mixed = jnp.transpose(mixed, (2, 0, 1, 3))
    screen = per_energy(screen_kernel, "screen", mixed, (coulomb,))
    screen = jnp.transpose(screen, (1, 2, 0, 3))
    (sigma,) = exchange(n, count, False, scale, (kept, screen, table, table_t))
    sigma = jnp.transpose(sigma, (2, 0, 1, 3))
    return per_energy(dyson_kernel, "dyson", sigma, (g_free,))


def solution(mesh):
    return jax.shard_map(
        functools.partial(per_device, mesh.shape["ea"], mesh.shape["bias"]),
        mesh=mesh,
        in_specs=(
            P(("bias", "ea"), None, None, None),
            P(("bias", "ea"), None, None, None),
            P(("bias", "ea"), None, None, None),
            P(),
        ),
        out_specs=P(("bias", "ea"), None, None, None),
        check_vma=False,
    )
```

```python
import functools
import math

import jax
import jax.numpy as jnp
import numpy as np
from jax import lax
from jax.experimental import pallas as pl
from jax.experimental.pallas import tpu as pltpu
from jax.sharding import PartitionSpec as P

NE = 256


def dft_tables(length, count):
    freq = jnp.arange(length, dtype=jnp.int32)
    places = jnp.arange(count, dtype=jnp.int32)
    phase = freq[:, None] * places[None, :] % length
    angle = phase.astype(jnp.float32) * (2.0 * math.pi / length)
    cosine = jnp.cos(angle)
    sine = jnp.sin(angle)
    stacked = jnp.concatenate([cosine, sine], axis=0)
    upper = stacked.astype(jnp.bfloat16)
    lower = (stacked - upper.astype(jnp.float32)).astype(jnp.bfloat16)
    backward = jnp.concatenate([cosine.T, sine.T], axis=0)
    return (upper, lower, backward)


def forward(tables, block, sign):
    upper, lower = tables
    length = upper.shape[0] // 2
    real_part = block[:, 0].reshape(block.shape[0], -1)
    imag_part = block[:, 1].reshape(block.shape[0], -1)
    width = real_part.shape[1]
    joined = jnp.concatenate([real_part, imag_part], axis=1)
    result = jnp.dot(upper, joined, preferred_element_type=jnp.float32)
    result = result + jnp.dot(lower, joined, preferred_element_type=jnp.float32)
    cos_real = result[:length, :width]
    cos_imag = result[:length, width:]
    sin_real = result[length:, :width]
    sin_imag = result[length:, width:]
    return (cos_real - sign * sin_imag, cos_imag + sign * sin_real)


def inverse(backward, real_part, imag_part, scale):
    count = backward.shape[0] // 2
    width = real_part.shape[1]
    joined = jnp.concatenate([real_part, imag_part], axis=1)
    result = jnp.dot(
        backward, joined, precision=lax.Precision.HIGH, preferred_element_type=jnp.float32
    )
    cos_real = result[:count, :width]
    cos_imag = result[:count, width:]
    sin_real = result[count:, :width]
    sin_imag = result[count:, width:]
    return ((cos_real - sin_imag) * scale, (cos_imag + sin_real) * scale)


def complex_mul(left, right):
    return (left[0] * right[0] - left[1] * right[1], left[0] * right[1] + left[1] * right[0])


def restack(real_part, imag_part, shape):
    return jnp.stack([real_part.reshape(shape), imag_part.reshape(shape)], axis=1).astype(
        jnp.bfloat16
    )


def batched(left, right):
    return jnp.einsum("eij,ejk->eik", left, right, preferred_element_type=jnp.float32)


def dyson(sigma_real, sigma_imag, g_free):
    free_real = g_free[:, 0]
    free_imag = g_free[:, 1]
    right_real = (batched(sigma_real, free_real) - batched(sigma_imag, free_imag)).astype(
        jnp.bfloat16
    )
    right_imag = (batched(sigma_real, free_imag) + batched(sigma_imag, free_real)).astype(
        jnp.bfloat16
    )
    out_real = (
        free_real.astype(jnp.float32)
        + batched(free_real, right_real)
        - batched(free_imag, right_imag)
    )
    out_imag = (
        free_imag.astype(jnp.float32)
        + batched(free_real, right_imag)
        + batched(free_imag, right_real)
    )
    return jnp.stack([out_real, out_imag], axis=1).astype(jnp.bfloat16)


def plain(g_lesser, g_greater, g_free, coulomb):
    length = 2 * NE
    upper, lower, backward = dft_tables(length, NE)
    tables = (upper, lower)
    scale = 1.0 / (length * NE)
    greater_t = jnp.swapaxes(g_greater, 2, 3)
    lesser_rows, greater_rows = (
        lax.all_to_all(g_lesser, "ea", split_axis=2, concat_axis=0, tiled=True),
        lax.all_to_all(greater_t, "ea", split_axis=2, concat_axis=0, tiled=True),
    )
    spec_lesser = forward(tables, lesser_rows, -1.0)
    element_shape = (NE, lesser_rows.shape[2], lesser_rows.shape[3])
    spec_greater = forward(tables, greater_rows, 1.0)
    joined = complex_mul(spec_lesser, spec_greater)
    polar_real, polar_imag = inverse(backward, joined[0], joined[1], scale)
    polar_rows = restack(polar_real, polar_imag, element_shape)
    polar = lax.all_to_all(polar_rows, "ea", split_axis=0, concat_axis=2, tiled=True)
    mixed_real = jnp.einsum(
        "eij,jk->eik", polar[:, 0], coulomb, preferred_element_type=jnp.float32
    ).astype(jnp.bfloat16)
    mixed_imag = jnp.einsum(
        "eij,jk->eik", polar[:, 1], coulomb, preferred_element_type=jnp.float32
    ).astype(jnp.bfloat16)
    square_real = batched(mixed_real, mixed_real) - batched(mixed_imag, mixed_imag)
    square_imag = batched(mixed_real, mixed_imag) + batched(mixed_imag, mixed_real)
    inner_real = (mixed_real.astype(jnp.float32) + square_real).astype(jnp.bfloat16)
    inner_imag = (mixed_imag.astype(jnp.float32) + square_imag).astype(jnp.bfloat16)
    screen_real = coulomb.astype(jnp.float32)[None] + jnp.einsum(
        "ij,ejk->eik", coulomb, inner_real, preferred_element_type=jnp.float32
    )
    screen_imag = jnp.einsum("ij,ejk->eik", coulomb, inner_imag, preferred_element_type=jnp.float32)
    screen = jnp.stack([screen_real, screen_imag], axis=1).astype(jnp.bfloat16)
    screen_rows = lax.all_to_all(screen, "ea", split_axis=2, concat_axis=0, tiled=True)
    spec_screen = forward(tables, screen_rows, -1.0)
    folded = complex_mul(spec_lesser, spec_screen)
    sigma_real, sigma_imag = inverse(backward, folded[0], folded[1], scale)
    sigma_rows = restack(sigma_real, sigma_imag, element_shape)
    sigma = lax.all_to_all(sigma_rows, "ea", split_axis=0, concat_axis=2, tiled=True)
    return dyson(sigma[:, 0], sigma[:, 1], g_free)


MESH = pl.DeviceIdType.MESH
CHUNKS = 8
AHEAD = 2
LANES = 128
VMEM_BYTES = 60 * 1024 * 1024


def transform_table(count):
    length = 2 * count
    phase = np.arange(length)[:, None] * np.arange(count)[None, :] % length
    angle = phase * (2.0 * math.pi / length)
    cosine, sine = np.cos(angle), np.sin(angle)
    return np.block([[cosine, sine], [-sine, cosine]]).astype(np.float32)


class Place:
    def __init__(self, n):
        self.n = n
        self.side = n // 2
        self.plane = lax.axis_index("bias")
        self.me = lax.axis_index("ea")
        self.half = lax.div(self.me, self.side)
        self.seat = lax.rem(self.me, self.side)
        self.member = self.plane * self.side + self.seat

    def of_member(self, member):
        return {
            "bias": lax.div(member, self.side),
            "ea": self.half * self.side + lax.rem(member, self.side),
        }


def greet(place):
    n = place.n
    barrier = pltpu.get_barrier_semaphore()
    mine = place.plane * n + place.me

    def hello(k, carry):
        other = lax.rem(mine + k, 2 * n)
        pl.semaphore_signal(
            barrier,
            inc=1,
            device_id={"bias": lax.div(other, n), "ea": lax.rem(other, n)},
            device_id_type=MESH,
        )
        return carry

    lax.fori_loop(1, 2 * n, hello, 0)
    pl.semaphore_wait(barrier, 2 * n - 1)


def loop(low, high, body):
    def step(k, carry):
        body(k)
        return carry

    lax.fori_loop(low, high, step, 0)


def fold_row(first, scale, count, table, table_t, lesser_buf, other_buf, folded, volts, row):
    length = 2 * count
    left = jnp.concatenate([lesser_buf[0, row], lesser_buf[1, row]], axis=0)
    imag = other_buf[1, row]
    right = jnp.concatenate([other_buf[0, row], -imag if first else imag], axis=0)
    left_spec = jnp.dot(table[...], left, preferred_element_type=jnp.float32)
    right_spec = jnp.dot(table[...], right, preferred_element_type=jnp.float32)
    left_real, left_imag = left_spec[:length], left_spec[length:]
    right_real, right_imag = right_spec[:length], right_spec[length:]
    if first:
        real = left_real * right_real + left_imag * right_imag
        imag = left_imag * right_real - left_real * right_imag
    else:
        real = left_real * right_real - left_imag * right_imag
        imag = left_real * right_imag + left_imag * right_real
    product = jnp.concatenate([real, imag], axis=0).astype(jnp.bfloat16)
    result = jnp.dot(table_t[...], product, preferred_element_type=jnp.float32) * scale
    result = result.astype(jnp.bfloat16)
    if first:
        result = jnp.dot(result, volts[...], preferred_element_type=jnp.float32)
        result = result.astype(jnp.bfloat16)
    folded[0, row] = result[:count]
    folded[1, row] = result[count:]


def polarize_kernel(
    n, count, scale, lesser, other, table, table_t, volts, out, kept,
    lesser_buf, other_buf, folded, in_send, in_recv, out_send, out_recv, own_in, own_out, keep,
    swap_send, swap_recv, lesser_raw, other_raw, lesser_rows, other_rows,
):
    place = Place(n)
    me, plane, half, side = place.me, place.plane, place.half, place.side
    rows = folded.shape[1]
    each = count // n
    group = rows // CHUNKS
    wide = side * group
    stages = (lesser_rows, other_rows)
    targets = (lesser_buf, other_buf)

    def swap(s, q):
        span = pl.ds(q * wide, wide)
        return pltpu.make_async_remote_copy(
            src_ref=stages[s].at[2, :, span],
            dst_ref=stages[s].at[plane, :, span],
            send_sem=swap_send.at[s, q],
            recv_sem=swap_recv.at[s, q],
            device_id={"bias": 1 - plane},
            device_id_type=MESH,
        )

    def ends(s, q, peer):
        source = stages[s].at[
            lax.div(peer, side), :, pl.ds(q * wide + lax.rem(peer, side) * group, group)
        ]
        target = targets[s].at[:, pl.ds(q * group, group), pl.ds(me * each, each)]
        return source, target

    def incoming(s, q, k):
        peer = lax.rem(me + k, n)
        source, target = ends(s, q, peer)
        return pltpu.make_async_remote_copy(
            src_ref=source,
            dst_ref=target,
            send_sem=in_send.at[s, q, k],
            recv_sem=in_recv.at[s, q, k],
            device_id={"ea": peer},
            device_id_type=MESH,
        )

    def own_incoming(s, q):
        source, target = ends(s, q, me)
        return pltpu.make_async_copy(source, target, own_in.at[s, q])

    def spread(s, q, bias):
        def send_one(j):
            peer = bias * side + lax.rem(place.seat + j, side)
            k = lax.rem(peer - me + n, n)

            @pl.when(k == 0)
            def _():
                own_incoming(s, q).start()

            @pl.when(k != 0)
            def _():
                incoming(s, q, k).start()

        loop(0, side, send_one)

    def outgoing(q, k):
        peer = lax.rem(place.member + k, n)
        return pltpu.make_async_remote_copy(
            src_ref=folded.at[:, pl.ds(q * group, group), pl.ds(peer * each, each)],
            dst_ref=out.at[:, pl.ds((q * n + place.member) * group, group)],
            send_sem=out_send.at[q, k],
            recv_sem=out_recv.at[q, k],
            device_id=place.of_member(peer),
            device_id_type=MESH,
        )

    def own_outgoing(q):
        return pltpu.make_async_copy(
            folded.at[:, pl.ds(q * group, group), pl.ds(place.member * each, each)],
            out.at[:, pl.ds((q * n + place.member) * group, group)],
            own_out.at[q],
        )

    raw = (
        pltpu.make_async_copy(lesser, lesser_raw, keep.at[0]),
        pltpu.make_async_copy(other, other_raw, keep.at[1]),
    )
    for copy in raw:
        copy.start()
    greet(place)
    raw[0].wait()

    def regroup(q):
        for h in range(2):
            slot = jnp.where(plane == h, h, 2)
            block = pl.ds(pl.multiple_of((2 * q + h) * wide, wide), wide)
            for c in range(2):
                lesser_rows[slot, c, pl.ds(pl.multiple_of(q * wide, wide), wide)] = jnp.swapaxes(
                    lesser_raw[:, c, block, :], 0, 1
                )
        swap(0, q).start()

    def turn(low):
        for c in range(2):
            turned = jnp.stack(
                [other_raw[e, c, :, low : low + LANES].T for e in range(each)], axis=0
            )
            turned = jnp.swapaxes(turned, 0, 1)
            for at in range(0, LANES, wide):
                piece = (low + at) // wide
                slot = jnp.where(plane == piece % 2, piece % 2, 2)
                start = piece // 2 * wide
                other_rows[slot, c, start : start + wide] = turned[at : at + wide]

    def relay(s, q):
        swap(s, q).wait_recv()
        spread(s, q, 1 - plane)

    def advance(q):
        for s in range(2):
            spread(s, q, plane)
            relay(s, q)

    def own_first(q):
        regroup(q)
        spread(0, q, plane)

    def both(q):
        regroup(q)
        swap(1, q).start()

    per = LANES // (2 * wide)
    loop(0, AHEAD, own_first)
    raw[1].wait()
    turn(0)
    loop(0, AHEAD, lambda q: swap(1, q).start())
    spread(1, 0, plane)
    loop(0, AHEAD, lambda q: relay(0, q))
    loop(AHEAD, per, both)
    for low in range(LANES, rows * n, LANES):
        turn(low)
        loop(low // LANES * per, (low // LANES + 1) * per, both)
    relay(1, 0)

    def rest(q):
        spread(1, q, plane)
        relay(1, q)

    loop(1, AHEAD, rest)

    def work(q):
        @pl.when(q + AHEAD < CHUNKS)
        def _():
            advance(q + AHEAD)

        for s in range(2):
            loop(1, n, lambda k: incoming(s, q, k).wait_recv())
            own_incoming(s, q).wait()
        loop(
            q * group,
            (q + 1) * group,
            functools.partial(
                fold_row, True, scale, count, table, table_t, lesser_buf, other_buf, folded, volts
            ),
        )
        loop(1, n, lambda k: outgoing(q, k).start())
        own_outgoing(q).start()

    loop(0, CHUNKS, work)
    keeping = pltpu.make_async_copy(lesser_buf, kept, keep.at[0])
    keeping.start()

    def finish(q):
        for s in range(2):
            swap(s, q).wait_send()
            loop(1, n, lambda k: incoming(s, q, k).wait_send())
        loop(1, n, lambda k: outgoing(q, k).wait())
        own_outgoing(q).wait()

    loop(0, CHUNKS, finish)
    keeping.wait()


def dress_kernel(
    n, count, scale, kept, screen, table, table_t, out,
    lesser_buf, other_buf, folded, in_send, in_recv, out_send, out_recv, own_in, own_out, keep,
):
    place = Place(n)
    me, plane, half = place.me, place.plane, place.half
    rows = folded.shape[1]
    each = count // n
    group = rows // CHUNKS

    def incoming(q, k):
        peer = lax.rem(place.member + k, n)
        return pltpu.make_async_remote_copy(
            src_ref=screen.at[:, pl.ds((q * n + peer) * group, group)],
            dst_ref=other_buf.at[:, pl.ds(q * group, group), pl.ds(place.member * each, each)],
            send_sem=in_send.at[q, k],
            recv_sem=in_recv.at[q, k],
            device_id=place.of_member(peer),
            device_id_type=MESH,
        )

    def own_incoming(q):
        return pltpu.make_async_copy(
            screen.at[:, pl.ds((q * n + place.member) * group, group)],
            other_buf.at[:, pl.ds(q * group, group), pl.ds(place.member * each, each)],
            own_in.at[q],
        )

    def outgoing(q, k, sender):
        peer = lax.rem(me + k, n)
        return pltpu.make_async_remote_copy(
            src_ref=folded.at[:, pl.ds(q * group, group), pl.ds(peer * each, each)],
            dst_ref=out.at[:, pl.ds((q * n + place.member) * group, group)],
            send_sem=out_send.at[q, k],
            recv_sem=out_recv.at[q, sender],
            device_id={"bias": half, "ea": peer},
            device_id_type=MESH,
        )

    def own_outgoing(q):
        return pltpu.make_async_copy(
            folded.at[:, pl.ds(q * group, group), pl.ds(me * each, each)],
            out.at[:, pl.ds((q * n + place.member) * group, group)],
            own_out.at[q],
        )

    at_home = plane == half
    keeping = pltpu.make_async_copy(kept, lesser_buf, keep.at[0])
    keeping.start()
    loop(0, CHUNKS, lambda q: own_incoming(q).start())
    greet(place)
    loop(0, CHUNKS, lambda q: loop(1, n, lambda k: incoming(q, k).start()))
    keeping.wait()

    def work(q):
        loop(1, n, lambda k: incoming(q, k).wait_recv())
        own_incoming(q).wait()
        loop(
            q * group,
            (q + 1) * group,
            functools.partial(
                fold_row, False, scale, count, table, table_t, lesser_buf, other_buf, folded, None
            ),
        )

        def far(j):
            peer = (1 - half) * place.side + lax.rem(place.seat + j, place.side)
            outgoing(q, lax.rem(peer - me + n, n), place.member).start()

        def near(j):
            peer = half * place.side + lax.rem(place.seat + j, place.side)
            outgoing(q, lax.rem(peer - me + n, n), place.member).start()

        loop(0, place.side, far)

        @pl.when(at_home)
        def _():
            own_outgoing(q).start()

        @pl.when(jnp.logical_not(at_home))
        def _():
            outgoing(q, 0, place.member).start()

        loop(1, place.side, near)

    loop(0, CHUNKS, work)

    def finish(q):
        loop(1, n, lambda k: incoming(q, k).wait_send())
        loop(1, n, lambda k: outgoing(q, k, place.member).wait_send())

        @pl.when(at_home)
        def _():
            own_outgoing(q).wait()

        @pl.when(jnp.logical_not(at_home))
        def _():
            outgoing(q, 0, place.member).wait_send()

        def wait_one(sender):
            @pl.when(jnp.logical_not(jnp.logical_and(at_home, sender == place.member)))
            def _():
                outgoing(q, 0, sender).wait_recv()

        loop(0, n, wait_one)

    loop(0, CHUNKS, finish)


def exchange(n, count, first, scale, operands):
    orbitals, width = operands[1].shape[-3 if not first else -2], operands[1].shape[-1]
    each = count // n
    rows = orbitals // n
    hbm = pl.BlockSpec(memory_space=pl.ANY)
    vmem = pl.BlockSpec(memory_space=pltpu.VMEM)
    out_shape = [jax.ShapeDtypeStruct((2, orbitals, each, width), jnp.bfloat16)]
    if first:
        out_shape.append(jax.ShapeDtypeStruct((2, rows, count, width), jnp.bfloat16))
    buffer = pltpu.VMEM((2, rows, count, width), jnp.bfloat16)
    dma = pltpu.SemaphoreType.DMA
    lead = (2, CHUNKS) if first else (CHUNKS,)
    scratch = [
        buffer, buffer, buffer,
        dma(lead + (n,)), dma(lead + (n,)), dma((CHUNKS, n)), dma((CHUNKS, n)),
        dma(lead), dma((CHUNKS,)), dma((2,)),
    ]
    if first:
        scratch += [dma((2, CHUNKS))] * 2
        scratch += [pltpu.VMEM((each, 2, orbitals, width), jnp.bfloat16)] * 2
        scratch += [pltpu.VMEM((3, 2, orbitals // 2, each, width), jnp.bfloat16)] * 2
    return pl.pallas_call(
        functools.partial(polarize_kernel if first else dress_kernel, n, count, scale),
        name="polarize" if first else "dress",
        out_shape=out_shape,
        in_specs=[hbm, hbm] + [vmem] * (len(operands) - 2),
        out_specs=[hbm] * len(out_shape),
        scratch_shapes=scratch,
        compiler_params=pltpu.CompilerParams(
            collective_id=0 if first else 1, has_side_effects=True, vmem_limit_bytes=VMEM_BYTES
        ),
    )(*operands)


def dot(left, right):
    return jnp.dot(left, right, preferred_element_type=jnp.float32)


def screen_kernel(mixed, volts, out):
    bare = volts[...]
    for e in range(mixed.shape[0]):
        real, imag = mixed[e, 0], mixed[e, 1]
        square_real = dot(real, real) - dot(imag, imag)
        square_imag = dot(real, imag) + dot(imag, real)
        inner_real = (real.astype(jnp.float32) + square_real).astype(jnp.bfloat16)
        inner_imag = (imag.astype(jnp.float32) + square_imag).astype(jnp.bfloat16)
        out[e, 0] = (bare.astype(jnp.float32) + dot(bare, inner_real)).astype(jnp.bfloat16)
        out[e, 1] = dot(bare, inner_imag).astype(jnp.bfloat16)


def dyson_kernel(sigma, free, out):
    for e in range(sigma.shape[0]):
        real, imag = sigma[e, 0], sigma[e, 1]
        free_real, free_imag = free[e, 0], free[e, 1]
        right_real = (dot(real, free_real) - dot(imag, free_imag)).astype(jnp.bfloat16)
        right_imag = (dot(real, free_imag) + dot(imag, free_real)).astype(jnp.bfloat16)
        out_real = dot(free_real, right_real) - dot(free_imag, right_imag)
        out_imag = dot(free_real, right_imag) + dot(free_imag, right_real)
        out[e, 0] = (free_real.astype(jnp.float32) + out_real).astype(jnp.bfloat16)
        out[e, 1] = (free_imag.astype(jnp.float32) + out_imag).astype(jnp.bfloat16)


def per_energy(kernel, name, matrices, others):
    each, two, rows, width = matrices.shape
    block = pl.BlockSpec((2, two, rows, width), lambda i: (i, 0, 0, 0))
    specs = [block if other.ndim == 4 else pl.BlockSpec(memory_space=pltpu.VMEM) for other in others]
    products = 6 if name == "screen" else 8
    return pl.pallas_call(
        kernel,
        name=name,
        grid=(each // 2,),
        out_shape=jax.ShapeDtypeStruct(matrices.shape, jnp.bfloat16),
        in_specs=[block] + specs,
        out_specs=block,
        cost_estimate=pl.CostEstimate(
            flops=2 * products * each * rows * rows * width,
            bytes_accessed=4 * two * each * rows * width,
            transcendentals=0,
        ),
    )(matrices, *others)


def per_device(n, biases, g_lesser, g_greater, g_free, coulomb):
    each, _, orbitals, _ = g_lesser.shape
    count = n * each
    if biases != 2 or n % 2 or each % 16 or orbitals % (n * 16) or LANES % (n // 2 * orbitals // n // CHUNKS):
        return plain(g_lesser, g_greater, g_free, coulomb)
    scale = 1.0 / (2 * count * count)
    full = transform_table(count)
    table = jnp.asarray(full).astype(jnp.bfloat16)
    table_t = jnp.asarray(full.T).astype(jnp.bfloat16)
    mixed, kept = exchange(n, count, True, scale, (g_lesser, g_greater, table, table_t, coulomb))
    mixed = jnp.transpose(mixed, (2, 0, 1, 3))
    screen = per_energy(screen_kernel, "screen", mixed, (coulomb,))
    screen = jnp.transpose(screen, (1, 2, 0, 3))
    (sigma,) = exchange(n, count, False, scale, (kept, screen, table, table_t))
    sigma = jnp.transpose(sigma, (2, 0, 1, 3))
    return per_energy(dyson_kernel, "dyson", sigma, (g_free,))


def solution(mesh):
    return jax.shard_map(
        functools.partial(per_device, mesh.shape["ea"], mesh.shape["bias"]),
        mesh=mesh,
        in_specs=(
            P(("bias", "ea"), None, None, None),
            P(("bias", "ea"), None, None, None),
            P(("bias", "ea"), None, None, None),
            P(),
        ),
        out_specs=P(("bias", "ea"), None, None, None),
        check_vma=False,
    )
```

```python
import functools
import math

import jax
import jax.numpy as jnp
import numpy as np
from jax import lax
from jax.experimental import pallas as pl
from jax.experimental.pallas import tpu as pltpu
from jax.sharding import PartitionSpec as P

NE = 256


def dft_tables(length, count):
    freq = jnp.arange(length, dtype=jnp.int32)
    places = jnp.arange(count, dtype=jnp.int32)
    phase = freq[:, None] * places[None, :] % length
    angle = phase.astype(jnp.float32) * (2.0 * math.pi / length)
    cosine = jnp.cos(angle)
    sine = jnp.sin(angle)
    stacked = jnp.concatenate([cosine, sine], axis=0)
    upper = stacked.astype(jnp.bfloat16)
    lower = (stacked - upper.astype(jnp.float32)).astype(jnp.bfloat16)
    backward = jnp.concatenate([cosine.T, sine.T], axis=0)
    return (upper, lower, backward)


def forward(tables, block, sign):
    upper, lower = tables
    length = upper.shape[0] // 2
    real_part = block[:, 0].reshape(block.shape[0], -1)
    imag_part = block[:, 1].reshape(block.shape[0], -1)
    width = real_part.shape[1]
    joined = jnp.concatenate([real_part, imag_part], axis=1)
    result = jnp.dot(upper, joined, preferred_element_type=jnp.float32)
    result = result + jnp.dot(lower, joined, preferred_element_type=jnp.float32)
    cos_real = result[:length, :width]
    cos_imag = result[:length, width:]
    sin_real = result[length:, :width]
    sin_imag = result[length:, width:]
    return (cos_real - sign * sin_imag, cos_imag + sign * sin_real)


def inverse(backward, real_part, imag_part, scale):
    count = backward.shape[0] // 2
    width = real_part.shape[1]
    joined = jnp.concatenate([real_part, imag_part], axis=1)
    result = jnp.dot(
        backward, joined, precision=lax.Precision.HIGH, preferred_element_type=jnp.float32
    )
    cos_real = result[:count, :width]
    cos_imag = result[:count, width:]
    sin_real = result[count:, :width]
    sin_imag = result[count:, width:]
    return ((cos_real - sin_imag) * scale, (cos_imag + sin_real) * scale)


def complex_mul(left, right):
    return (left[0] * right[0] - left[1] * right[1], left[0] * right[1] + left[1] * right[0])


def restack(real_part, imag_part, shape):
    return jnp.stack([real_part.reshape(shape), imag_part.reshape(shape)], axis=1).astype(
        jnp.bfloat16
    )


def batched(left, right):
    return jnp.einsum("eij,ejk->eik", left, right, preferred_element_type=jnp.float32)


def dyson(sigma_real, sigma_imag, g_free):
    free_real = g_free[:, 0]
    free_imag = g_free[:, 1]
    right_real = (batched(sigma_real, free_real) - batched(sigma_imag, free_imag)).astype(
        jnp.bfloat16
    )
    right_imag = (batched(sigma_real, free_imag) + batched(sigma_imag, free_real)).astype(
        jnp.bfloat16
    )
    out_real = (
        free_real.astype(jnp.float32)
        + batched(free_real, right_real)
        - batched(free_imag, right_imag)
    )
    out_imag = (
        free_imag.astype(jnp.float32)
        + batched(free_real, right_imag)
        + batched(free_imag, right_real)
    )
    return jnp.stack([out_real, out_imag], axis=1).astype(jnp.bfloat16)


def plain(g_lesser, g_greater, g_free, coulomb):
    length = 2 * NE
    upper, lower, backward = dft_tables(length, NE)
    tables = (upper, lower)
    scale = 1.0 / (length * NE)
    greater_t = jnp.swapaxes(g_greater, 2, 3)
    lesser_rows, greater_rows = (
        lax.all_to_all(g_lesser, "ea", split_axis=2, concat_axis=0, tiled=True),
        lax.all_to_all(greater_t, "ea", split_axis=2, concat_axis=0, tiled=True),
    )
    spec_lesser = forward(tables, lesser_rows, -1.0)
    element_shape = (NE, lesser_rows.shape[2], lesser_rows.shape[3])
    spec_greater = forward(tables, greater_rows, 1.0)
    joined = complex_mul(spec_lesser, spec_greater)
    polar_real, polar_imag = inverse(backward, joined[0], joined[1], scale)
    polar_rows = restack(polar_real, polar_imag, element_shape)
    polar = lax.all_to_all(polar_rows, "ea", split_axis=0, concat_axis=2, tiled=True)
    mixed_real = jnp.einsum(
        "eij,jk->eik", polar[:, 0], coulomb, preferred_element_type=jnp.float32
    ).astype(jnp.bfloat16)
    mixed_imag = jnp.einsum(
        "eij,jk->eik", polar[:, 1], coulomb, preferred_element_type=jnp.float32
    ).astype(jnp.bfloat16)
    square_real = batched(mixed_real, mixed_real) - batched(mixed_imag, mixed_imag)
    square_imag = batched(mixed_real, mixed_imag) + batched(mixed_imag, mixed_real)
    inner_real = (mixed_real.astype(jnp.float32) + square_real).astype(jnp.bfloat16)
    inner_imag = (mixed_imag.astype(jnp.float32) + square_imag).astype(jnp.bfloat16)
    screen_real = coulomb.astype(jnp.float32)[None] + jnp.einsum(
        "ij,ejk->eik", coulomb, inner_real, preferred_element_type=jnp.float32
    )
    screen_imag = jnp.einsum("ij,ejk->eik", coulomb, inner_imag, preferred_element_type=jnp.float32)
    screen = jnp.stack([screen_real, screen_imag], axis=1).astype(jnp.bfloat16)
    screen_rows = lax.all_to_all(screen, "ea", split_axis=2, concat_axis=0, tiled=True)
    spec_screen = forward(tables, screen_rows, -1.0)
    folded = complex_mul(spec_lesser, spec_screen)
    sigma_real, sigma_imag = inverse(backward, folded[0], folded[1], scale)
    sigma_rows = restack(sigma_real, sigma_imag, element_shape)
    sigma = lax.all_to_all(sigma_rows, "ea", split_axis=0, concat_axis=2, tiled=True)
    return dyson(sigma[:, 0], sigma[:, 1], g_free)


MESH = pl.DeviceIdType.MESH
CHUNKS = 8
AHEAD = 2
BEHIND = 2
LANES = 128
VMEM_BYTES = 60 * 1024 * 1024


def transform_table(count):
    length = 2 * count
    phase = np.arange(length)[:, None] * np.arange(count)[None, :] % length
    angle = phase * (2.0 * math.pi / length)
    cosine, sine = np.cos(angle), np.sin(angle)
    return np.block([[cosine, sine], [-sine, cosine]]).astype(np.float32)


class Place:
    def __init__(self, n):
        self.n = n
        self.side = n // 2
        self.plane = lax.axis_index("bias")
        self.me = lax.axis_index("ea")
        self.half = lax.div(self.me, self.side)
        self.seat = lax.rem(self.me, self.side)
        self.member = self.plane * self.side + self.seat

    def of_member(self, member):
        return {
            "bias": lax.div(member, self.side),
            "ea": self.half * self.side + lax.rem(member, self.side),
        }


def greet(place):
    n = place.n
    barrier = pltpu.get_barrier_semaphore()
    mine = place.plane * n + place.me

    def hello(k, carry):
        other = lax.rem(mine + k, 2 * n)
        pl.semaphore_signal(
            barrier,
            inc=1,
            device_id={"bias": lax.div(other, n), "ea": lax.rem(other, n)},
            device_id_type=MESH,
        )
        return carry

    lax.fori_loop(1, 2 * n, hello, 0)
    pl.semaphore_wait(barrier, 2 * n - 1)


def loop(low, high, body):
    def step(k, carry):
        body(k)
        return carry

    lax.fori_loop(low, high, step, 0)


def fold_row(first, scale, count, table, table_t, lesser_buf, other_buf, folded, volts, row):
    length = 2 * count
    left = jnp.concatenate([lesser_buf[0, row], lesser_buf[1, row]], axis=0)
    imag = other_buf[1, row]
    right = jnp.concatenate([other_buf[0, row], -imag if first else imag], axis=0)
    left_spec = jnp.dot(table[...], left, preferred_element_type=jnp.float32)
    right_spec = jnp.dot(table[...], right, preferred_element_type=jnp.float32)
    left_real, left_imag = left_spec[:length], left_spec[length:]
    right_real, right_imag = right_spec[:length], right_spec[length:]
    if first:
        real = left_real * right_real + left_imag * right_imag
        imag = left_imag * right_real - left_real * right_imag
    else:
        real = left_real * right_real - left_imag * right_imag
        imag = left_real * right_imag + left_imag * right_real
    product = jnp.concatenate([real, imag], axis=0).astype(jnp.bfloat16)
    result = jnp.dot(table_t[...], product, preferred_element_type=jnp.float32) * scale
    result = result.astype(jnp.bfloat16)
    if first:
        result = jnp.dot(result, volts[...], preferred_element_type=jnp.float32)
        result = result.astype(jnp.bfloat16)
    folded[0, row] = result[:count]
    folded[1, row] = result[count:]


def gw_kernel(
    n, count, scale, lesser, other, table, table_t, volts, out,
    lesser_buf, other_buf, folded, lesser_raw, other_raw, lesser_rows, other_rows,
    mixed, screen, sigma,
    in_send, in_recv, own_in, swap_send, swap_recv, p_send, p_recv, p_own,
    w_send, w_recv, w_own, s_send, s_recv, s_own, keep,
):
    place = Place(n)
    me, plane, half, side = place.me, place.plane, place.half, place.side
    member = place.member
    rows = folded.shape[1]
    each = count // n
    group = rows // CHUNKS
    wide = side * group
    stages = (lesser_rows, other_rows)
    targets = (lesser_buf, other_buf)
    at_home = plane == half

    def swap(s, q):
        span = pl.ds(q * wide, wide)
        return pltpu.make_async_remote_copy(
            src_ref=stages[s].at[2, :, span],
            dst_ref=stages[s].at[plane, :, span],
            send_sem=swap_send.at[s, q],
            recv_sem=swap_recv.at[s, q],
            device_id={"bias": 1 - plane},
            device_id_type=MESH,
        )

    def ends(s, q, peer):
        source = stages[s].at[
            lax.div(peer, side), :, pl.ds(q * wide + lax.rem(peer, side) * group, group)
        ]
        target = targets[s].at[:, pl.ds(q * group, group), pl.ds(me * each, each)]
        return source, target

    def incoming(s, q, k):
        peer = lax.rem(me + k, n)
        source, target = ends(s, q, peer)
        return pltpu.make_async_remote_copy(
            src_ref=source,
            dst_ref=target,
            send_sem=in_send.at[s, q, k],
            recv_sem=in_recv.at[s, q, k],
            device_id={"ea": peer},
            device_id_type=MESH,
        )

    def own_incoming(s, q):
        source, target = ends(s, q, me)
        return pltpu.make_async_copy(source, target, own_in.at[s, q])

    def spread(s, q, bias):
        def send_one(j):
            peer = bias * side + lax.rem(place.seat + j, side)
            k = lax.rem(peer - me + n, n)

            @pl.when(k == 0)
            def _():
                own_incoming(s, q).start()

            @pl.when(k != 0)
            def _():
                incoming(s, q, k).start()

        loop(0, side, send_one)

    def mine(q):
        return pl.ds((q * n + member) * group, group)

    def polar(q, k):
        peer = lax.rem(member + k, n)
        return pltpu.make_async_remote_copy(
            src_ref=folded.at[:, pl.ds(q * group, group), pl.ds(peer * each, each)],
            dst_ref=mixed.at[:, mine(q)],
            send_sem=p_send.at[q, k],
            recv_sem=p_recv.at[q, k],
            device_id=place.of_member(peer),
            device_id_type=MESH,
        )

    def own_polar(q):
        return pltpu.make_async_copy(
            folded.at[:, pl.ds(q * group, group), pl.ds(member * each, each)],
            mixed.at[:, mine(q)],
            p_own.at[q],
        )

    def screened(q, k):
        peer = lax.rem(member + k, n)
        return pltpu.make_async_remote_copy(
            src_ref=screen.at[:, pl.ds((q * n + peer) * group, group)],
            dst_ref=other_buf.at[:, pl.ds(q * group, group), pl.ds(member * each, each)],
            send_sem=w_send.at[q, k],
            recv_sem=w_recv.at[q, k],
            device_id=place.of_member(peer),
            device_id_type=MESH,
        )

    def own_screened(q):
        return pltpu.make_async_copy(
            screen.at[:, mine(q)],
            other_buf.at[:, pl.ds(q * group, group), pl.ds(member * each, each)],
            w_own.at[q],
        )

    def dressed(q, k, sender):
        peer = lax.rem(me + k, n)
        return pltpu.make_async_remote_copy(
            src_ref=folded.at[:, pl.ds(q * group, group), pl.ds(peer * each, each)],
            dst_ref=sigma.at[:, mine(q)],
            send_sem=s_send.at[q, k],
            recv_sem=s_recv.at[q, sender],
            device_id={"bias": half, "ea": peer},
            device_id_type=MESH,
        )

    def own_dressed(q):
        return pltpu.make_async_copy(
            folded.at[:, pl.ds(q * group, group), pl.ds(me * each, each)],
            sigma.at[:, mine(q)],
            s_own.at[q],
        )

    raw = (
        pltpu.make_async_copy(lesser, lesser_raw, keep.at[0]),
        pltpu.make_async_copy(other, other_raw, keep.at[1]),
    )
    for copy in raw:
        copy.start()
    greet(place)
    raw[0].wait()

    def regroup(q):
        for h in range(2):
            slot = jnp.where(plane == h, h, 2)
            block = pl.ds(pl.multiple_of((2 * q + h) * wide, wide), wide)
            for c in range(2):
                lesser_rows[slot, c, pl.ds(pl.multiple_of(q * wide, wide), wide)] = jnp.swapaxes(
                    lesser_raw[:, c, block, :], 0, 1
                )
        swap(0, q).start()

    def turn(low):
        for c in range(2):
            turned = jnp.stack(
                [other_raw[e, c, :, low : low + LANES].T for e in range(each)], axis=0
            )
            turned = jnp.swapaxes(turned, 0, 1)
            for at in range(0, LANES, wide):
                piece = (low + at) // wide
                slot = jnp.where(plane == piece % 2, piece % 2, 2)
                start = piece // 2 * wide
                other_rows[slot, c, start : start + wide] = turned[at : at + wide]

    def relay(s, q):
        swap(s, q).wait_recv()
        spread(s, q, 1 - plane)

    def advance(q):
        for s in range(2):
            spread(s, q, plane)
            relay(s, q)

    def own_first(q):
        regroup(q)
        spread(0, q, plane)

    def both(q):
        regroup(q)
        swap(1, q).start()

    per = LANES // (2 * wide)
    loop(0, AHEAD, own_first)
    raw[1].wait()
    turn(0)
    loop(0, AHEAD, lambda q: swap(1, q).start())
    spread(1, 0, plane)
    loop(0, AHEAD, lambda q: relay(0, q))
    loop(AHEAD, per, both)
    for low in range(LANES, rows * n, LANES):
        turn(low)
        loop(low // LANES * per, (low // LANES + 1) * per, both)
    relay(1, 0)

    def rest(q):
        spread(1, q, plane)
        relay(1, q)

    loop(1, AHEAD, rest)

    def chunk_rows(q):
        return pl.ds(pl.multiple_of(q * 2 * wide, 2 * wide), 2 * wide)

    def absorb(q):
        loop(1, n, lambda k: polar(q, k).wait_recv())
        own_polar(q).wait()
        for c in range(2):
            lesser_raw[:, c, chunk_rows(q), :] = jnp.swapaxes(mixed[c, chunk_rows(q)], 0, 1)

    def work(q):
        @pl.when(q + AHEAD < CHUNKS)
        def _():
            advance(q + AHEAD)

        for s in range(2):
            loop(1, n, lambda k: incoming(s, q, k).wait_recv())
            own_incoming(s, q).wait()
        loop(
            q * group,
            (q + 1) * group,
            functools.partial(
                fold_row, True, scale, count, table, table_t, lesser_buf, other_buf, folded, volts
            ),
        )
        loop(1, n, lambda k: polar(q, k).start())
        own_polar(q).start()

        @pl.when(q >= BEHIND)
        def _():
            absorb(q - BEHIND)

    loop(0, CHUNKS, work)
    loop(CHUNKS - BEHIND, CHUNKS, absorb)
    bare = volts[...]
    width = bare.shape[0]

    def screen_one(e):
        pair = lesser_raw[e].reshape(2 * width, width)
        by_real = dot(pair, lesser_raw[e, 0])
        by_imag = dot(pair, lesser_raw[e, 1])
        square_real = by_real[:width] - by_imag[width:]
        square_imag = by_imag[:width] + by_real[width:]
        inner = jnp.concatenate(
            [
                (lesser_raw[e, 0].astype(jnp.float32) + square_real).astype(jnp.bfloat16),
                (lesser_raw[e, 1].astype(jnp.float32) + square_imag).astype(jnp.bfloat16),
            ],
            axis=1,
        )
        result = dot(bare, inner)
        lesser_raw[e, 0] = (bare.astype(jnp.float32) + result[:, :width]).astype(jnp.bfloat16)
        lesser_raw[e, 1] = result[:, width:].astype(jnp.bfloat16)

    loop(0, each, screen_one)

    def send_screen(q):
        for c in range(2):
            screen[c, chunk_rows(q)] = jnp.swapaxes(lesser_raw[:, c, chunk_rows(q), :], 0, 1)
        loop(1, n, lambda k: screened(q, k).start())
        own_screened(q).start()

    loop(0, CHUNKS, send_screen)

    def settle(q):
        for s in range(2):
            swap(s, q).wait_send()
            loop(1, n, lambda k: incoming(s, q, k).wait_send())
        loop(1, n, lambda k: polar(q, k).wait_send())

    loop(0, CHUNKS, settle)

    def dress(q):
        loop(1, n, lambda k: screened(q, k).wait_recv())
        own_screened(q).wait()
        loop(
            q * group,
            (q + 1) * group,
            functools.partial(
                fold_row, False, scale, count, table, table_t, lesser_buf, other_buf, folded, None
            ),
        )

        def send_to(target_half):
            def send_one(j):
                peer = target_half * side + lax.rem(place.seat + j, side)
                dressed(q, lax.rem(peer - me + n, n), member).start()

            return send_one

        loop(0, side, send_to(1 - half))

        @pl.when(at_home)
        def _():
            own_dressed(q).start()

        @pl.when(jnp.logical_not(at_home))
        def _():
            dressed(q, 0, member).start()

        loop(1, side, send_to(half))

    loop(0, CHUNKS, dress)

    def collect(q):
        @pl.when(at_home)
        def _():
            own_dressed(q).wait()

        def wait_one(sender):
            @pl.when(jnp.logical_not(jnp.logical_and(at_home, sender == member)))
            def _():
                dressed(q, 0, sender).wait_recv()

        loop(0, n, wait_one)
        for c in range(2):
            lesser_raw[:, c, chunk_rows(q), :] = jnp.swapaxes(sigma[c, chunk_rows(q)], 0, 1)

    loop(0, CHUNKS, collect)
    result = pltpu.make_async_copy(lesser_raw, out, keep.at[0])
    result.start()

    def finish(q):
        loop(1, n, lambda k: screened(q, k).wait_send())
        loop(1, n, lambda k: dressed(q, k, member).wait_send())

        @pl.when(jnp.logical_not(at_home))
        def _():
            dressed(q, 0, member).wait_send()

    loop(0, CHUNKS, finish)
    result.wait()


def iterate(n, count, scale, g_lesser, g_greater, table, table_t, coulomb):
    each, _, orbitals, width = g_lesser.shape
    rows = orbitals // n
    hbm = pl.BlockSpec(memory_space=pl.ANY)
    vmem = pl.BlockSpec(memory_space=pltpu.VMEM)
    by_row = pltpu.VMEM((2, rows, count, width), jnp.bfloat16)
    by_energy = pltpu.VMEM((each, 2, orbitals, width), jnp.bfloat16)
    stage = pltpu.VMEM((3, 2, orbitals // 2, each, width), jnp.bfloat16)
    landing = pltpu.VMEM((2, orbitals, each, width), jnp.bfloat16)
    dma = pltpu.SemaphoreType.DMA
    pairs = dma((CHUNKS, n))
    return pl.pallas_call(
        functools.partial(gw_kernel, n, count, scale),
        name="iterate",
        out_shape=jax.ShapeDtypeStruct(g_lesser.shape, jnp.bfloat16),
        in_specs=[hbm, hbm, vmem, vmem, vmem],
        out_specs=hbm,
        scratch_shapes=[
            by_row, by_row, by_row, by_energy, by_energy, stage, stage,
            landing, landing, landing,
            dma((2, CHUNKS, n)), dma((2, CHUNKS, n)), dma((2, CHUNKS)),
            dma((2, CHUNKS)), dma((2, CHUNKS)),
            pairs, pairs, dma((CHUNKS,)),
            pairs, pairs, dma((CHUNKS,)),
            pairs, pairs, dma((CHUNKS,)), dma((2,)),
        ],
        compiler_params=pltpu.CompilerParams(
            collective_id=0, has_side_effects=True, vmem_limit_bytes=VMEM_BYTES
        ),
    )(g_lesser, g_greater, table, table_t, coulomb)


def dot(left, right):
    return jnp.dot(left, right, preferred_element_type=jnp.float32)


def dyson_kernel(sigma, free, out):
    for e in range(sigma.shape[0]):
        real, imag = sigma[e, 0], sigma[e, 1]
        free_real, free_imag = free[e, 0], free[e, 1]
        right_real = (dot(real, free_real) - dot(imag, free_imag)).astype(jnp.bfloat16)
        right_imag = (dot(real, free_imag) + dot(imag, free_real)).astype(jnp.bfloat16)
        out_real = dot(free_real, right_real) - dot(free_imag, right_imag)
        out_imag = dot(free_real, right_imag) + dot(free_imag, right_real)
        out[e, 0] = (free_real.astype(jnp.float32) + out_real).astype(jnp.bfloat16)
        out[e, 1] = (free_imag.astype(jnp.float32) + out_imag).astype(jnp.bfloat16)


def per_energy(kernel, name, matrices, others):
    each, two, rows, width = matrices.shape
    block = pl.BlockSpec((2, two, rows, width), lambda i: (i, 0, 0, 0))
    specs = [block if other.ndim == 4 else pl.BlockSpec(memory_space=pltpu.VMEM) for other in others]
    products = 6 if name == "screen" else 8
    return pl.pallas_call(
        kernel,
        name=name,
        grid=(each // 2,),
        out_shape=jax.ShapeDtypeStruct(matrices.shape, jnp.bfloat16),
        in_specs=[block] + specs,
        out_specs=block,
        cost_estimate=pl.CostEstimate(
            flops=2 * products * each * rows * rows * width,
            bytes_accessed=4 * two * each * rows * width,
            transcendentals=0,
        ),
    )(matrices, *others)


def per_device(n, biases, g_lesser, g_greater, g_free, coulomb):
    each, _, orbitals, _ = g_lesser.shape
    count = n * each
    if biases != 2 or n % 2 or each % 16 or orbitals % (n * 16) or LANES % (n // 2 * orbitals // n // CHUNKS):
        return plain(g_lesser, g_greater, g_free, coulomb)
    scale = 1.0 / (2 * count * count)
    full = transform_table(count)
    table = jnp.asarray(full).astype(jnp.bfloat16)
    table_t = jnp.asarray(full.T).astype(jnp.bfloat16)
    sigma = iterate(n, count, scale, g_lesser, g_greater, table, table_t, coulomb)
    return per_energy(dyson_kernel, "dyson", sigma, (g_free,))


def solution(mesh):
    return jax.shard_map(
        functools.partial(per_device, mesh.shape["ea"], mesh.shape["bias"]),
        mesh=mesh,
        in_specs=(
            P(("bias", "ea"), None, None, None),
            P(("bias", "ea"), None, None, None),
            P(("bias", "ea"), None, None, None),
            P(),
        ),
        out_specs=P(("bias", "ea"), None, None, None),
        check_vma=False,
    )
```

```python
import functools
import math

import jax
import jax.numpy as jnp
import numpy as np
from jax import lax
from jax.experimental import pallas as pl
from jax.experimental.pallas import tpu as pltpu
from jax.sharding import PartitionSpec as P

NE = 256


def dft_tables(length, count):
    freq = jnp.arange(length, dtype=jnp.int32)
    places = jnp.arange(count, dtype=jnp.int32)
    phase = freq[:, None] * places[None, :] % length
    angle = phase.astype(jnp.float32) * (2.0 * math.pi / length)
    cosine = jnp.cos(angle)
    sine = jnp.sin(angle)
    stacked = jnp.concatenate([cosine, sine], axis=0)
    upper = stacked.astype(jnp.bfloat16)
    lower = (stacked - upper.astype(jnp.float32)).astype(jnp.bfloat16)
    backward = jnp.concatenate([cosine.T, sine.T], axis=0)
    return (upper, lower, backward)


def forward(tables, block, sign):
    upper, lower = tables
    length = upper.shape[0] // 2
    real_part = block[:, 0].reshape(block.shape[0], -1)
    imag_part = block[:, 1].reshape(block.shape[0], -1)
    width = real_part.shape[1]
    joined = jnp.concatenate([real_part, imag_part], axis=1)
    result = jnp.dot(upper, joined, preferred_element_type=jnp.float32)
    result = result + jnp.dot(lower, joined, preferred_element_type=jnp.float32)
    cos_real = result[:length, :width]
    cos_imag = result[:length, width:]
    sin_real = result[length:, :width]
    sin_imag = result[length:, width:]
    return (cos_real - sign * sin_imag, cos_imag + sign * sin_real)


def inverse(backward, real_part, imag_part, scale):
    count = backward.shape[0] // 2
    width = real_part.shape[1]
    joined = jnp.concatenate([real_part, imag_part], axis=1)
    result = jnp.dot(
        backward, joined, precision=lax.Precision.HIGH, preferred_element_type=jnp.float32
    )
    cos_real = result[:count, :width]
    cos_imag = result[:count, width:]
    sin_real = result[count:, :width]
    sin_imag = result[count:, width:]
    return ((cos_real - sin_imag) * scale, (cos_imag + sin_real) * scale)


def complex_mul(left, right):
    return (left[0] * right[0] - left[1] * right[1], left[0] * right[1] + left[1] * right[0])


def restack(real_part, imag_part, shape):
    return jnp.stack([real_part.reshape(shape), imag_part.reshape(shape)], axis=1).astype(
        jnp.bfloat16
    )


def batched(left, right):
    return jnp.einsum("eij,ejk->eik", left, right, preferred_element_type=jnp.float32)


def dyson(sigma_real, sigma_imag, g_free):
    free_real = g_free[:, 0]
    free_imag = g_free[:, 1]
    right_real = (batched(sigma_real, free_real) - batched(sigma_imag, free_imag)).astype(
        jnp.bfloat16
    )
    right_imag = (batched(sigma_real, free_imag) + batched(sigma_imag, free_real)).astype(
        jnp.bfloat16
    )
    out_real = (
        free_real.astype(jnp.float32)
        + batched(free_real, right_real)
        - batched(free_imag, right_imag)
    )
    out_imag = (
        free_imag.astype(jnp.float32)
        + batched(free_real, right_imag)
        + batched(free_imag, right_real)
    )
    return jnp.stack([out_real, out_imag], axis=1).astype(jnp.bfloat16)


def plain(g_lesser, g_greater, g_free, coulomb):
    length = 2 * NE
    upper, lower, backward = dft_tables(length, NE)
    tables = (upper, lower)
    scale = 1.0 / (length * NE)
    greater_t = jnp.swapaxes(g_greater, 2, 3)
    lesser_rows, greater_rows = (
        lax.all_to_all(g_lesser, "ea", split_axis=2, concat_axis=0, tiled=True),
        lax.all_to_all(greater_t, "ea", split_axis=2, concat_axis=0, tiled=True),
    )
    spec_lesser = forward(tables, lesser_rows, -1.0)
    element_shape = (NE, lesser_rows.shape[2], lesser_rows.shape[3])
    spec_greater = forward(tables, greater_rows, 1.0)
    joined = complex_mul(spec_lesser, spec_greater)
    polar_real, polar_imag = inverse(backward, joined[0], joined[1], scale)
    polar_rows = restack(polar_real, polar_imag, element_shape)
    polar = lax.all_to_all(polar_rows, "ea", split_axis=0, concat_axis=2, tiled=True)
    mixed_real = jnp.einsum(
        "eij,jk->eik", polar[:, 0], coulomb, preferred_element_type=jnp.float32
    ).astype(jnp.bfloat16)
    mixed_imag = jnp.einsum(
        "eij,jk->eik", polar[:, 1], coulomb, preferred_element_type=jnp.float32
    ).astype(jnp.bfloat16)
    square_real = batched(mixed_real, mixed_real) - batched(mixed_imag, mixed_imag)
    square_imag = batched(mixed_real, mixed_imag) + batched(mixed_imag, mixed_real)
    inner_real = (mixed_real.astype(jnp.float32) + square_real).astype(jnp.bfloat16)
    inner_imag = (mixed_imag.astype(jnp.float32) + square_imag).astype(jnp.bfloat16)
    screen_real = coulomb.astype(jnp.float32)[None] + jnp.einsum(
        "ij,ejk->eik", coulomb, inner_real, preferred_element_type=jnp.float32
    )
    screen_imag = jnp.einsum("ij,ejk->eik", coulomb, inner_imag, preferred_element_type=jnp.float32)
    screen = jnp.stack([screen_real, screen_imag], axis=1).astype(jnp.bfloat16)
    screen_rows = lax.all_to_all(screen, "ea", split_axis=2, concat_axis=0, tiled=True)
    spec_screen = forward(tables, screen_rows, -1.0)
    folded = complex_mul(spec_lesser, spec_screen)
    sigma_real, sigma_imag = inverse(backward, folded[0], folded[1], scale)
    sigma_rows = restack(sigma_real, sigma_imag, element_shape)
    sigma = lax.all_to_all(sigma_rows, "ea", split_axis=0, concat_axis=2, tiled=True)
    return dyson(sigma[:, 0], sigma[:, 1], g_free)


MESH = pl.DeviceIdType.MESH
CHUNKS = 16
AHEAD = 6
BEHIND = 4
UNROLL = 4
LANES = 128
VMEM_BYTES = 60 * 1024 * 1024


def transform_table(count):
    length = 2 * count
    phase = np.arange(length)[:, None] * np.arange(count)[None, :] % length
    angle = phase * (2.0 * math.pi / length)
    cosine, sine = np.cos(angle), np.sin(angle)
    return np.block([[cosine, sine], [-sine, cosine]]).astype(np.float32)


class Place:
    def __init__(self, n):
        self.n = n
        self.side = n // 2
        self.plane = lax.axis_index("bias")
        self.me = lax.axis_index("ea")
        self.half = lax.div(self.me, self.side)
        self.seat = lax.rem(self.me, self.side)
        self.member = self.plane * self.side + self.seat

    def of_member(self, member):
        return {
            "bias": lax.div(member, self.side),
            "ea": self.half * self.side + lax.rem(member, self.side),
        }


def greet(place):
    n = place.n
    barrier = pltpu.get_barrier_semaphore()
    mine = place.plane * n + place.me

    def hello(k, carry):
        other = lax.rem(mine + k, 2 * n)
        pl.semaphore_signal(
            barrier,
            inc=1,
            device_id={"bias": lax.div(other, n), "ea": lax.rem(other, n)},
            device_id_type=MESH,
        )
        return carry

    lax.fori_loop(1, 2 * n, hello, 0)
    pl.semaphore_wait(barrier, 2 * n - 1)


def loop(low, high, body):
    def step(k, carry):
        body(k)
        return carry

    lax.fori_loop(low, high, step, 0)


def fold_row(first, scale, count, table, table_t, lesser_buf, other_buf, folded, volts, row):
    length = 2 * count
    left = jnp.concatenate([lesser_buf[0, row], lesser_buf[1, row]], axis=0)
    imag = other_buf[1, row]
    right = jnp.concatenate([other_buf[0, row], -imag if first else imag], axis=0)
    left_spec = jnp.dot(table[...], left, preferred_element_type=jnp.float32)
    right_spec = jnp.dot(table[...], right, preferred_element_type=jnp.float32)
    left_real, left_imag = left_spec[:length], left_spec[length:]
    right_real, right_imag = right_spec[:length], right_spec[length:]
    if first:
        real = left_real * right_real + left_imag * right_imag
        imag = left_imag * right_real - left_real * right_imag
    else:
        real = left_real * right_real - left_imag * right_imag
        imag = left_real * right_imag + left_imag * right_real
    product = jnp.concatenate([real, imag], axis=0).astype(jnp.bfloat16)
    result = jnp.dot(table_t[...], product, preferred_element_type=jnp.float32) * scale
    result = result.astype(jnp.bfloat16)
    if first:
        result = jnp.dot(result, volts[...], preferred_element_type=jnp.float32)
        result = result.astype(jnp.bfloat16)
    folded[0, row] = result[:count]
    folded[1, row] = result[count:]


def gw_kernel(
    n, count, scale, lesser, other, table, table_t, volts, out,
    lesser_buf, other_buf, folded, lesser_raw, other_raw, lesser_rows, other_rows,
    mixed, screen, sigma,
    in_send, in_recv, swap_send, swap_recv, p_send, p_recv, w_send, w_recv, s_send, s_recv, keep,
):
    place = Place(n)
    me, plane, half, side = place.me, place.plane, place.half, place.side
    member = place.member
    rows = folded.shape[1]
    each = count // n
    group = rows // CHUNKS
    wide = side * group
    stages = (lesser_rows, other_rows)
    targets = (lesser_buf, other_buf)
    at_home = plane == half

    def swap(s, q):
        span = pl.ds(q * wide, wide)
        return pltpu.make_async_remote_copy(
            src_ref=stages[s].at[2, :, span],
            dst_ref=stages[s].at[plane, :, span],
            send_sem=swap_send.at[s, q],
            recv_sem=swap_recv.at[s, q],
            device_id={"bias": 1 - plane},
            device_id_type=MESH,
        )

    def ends(s, q, peer):
        source = stages[s].at[
            lax.div(peer, side), :, pl.ds(q * wide + lax.rem(peer, side) * group, group)
        ]
        target = targets[s].at[:, pl.ds(q * group, group), pl.ds(me * each, each)]
        return source, target

    def incoming(s, q, k):
        peer = lax.rem(me + k, n)
        source, target = ends(s, q, peer)
        return pltpu.make_async_remote_copy(
            src_ref=source,
            dst_ref=target,
            send_sem=in_send.at[s, q],
            recv_sem=in_recv.at[s, q],
            device_id={"ea": peer},
            device_id_type=MESH,
        )

    def own_incoming(s, q):
        source, target = ends(s, q, me)
        return pltpu.make_async_copy(source, target, in_recv.at[s, q])

    def spread(s, q, bias):
        def send_one(j):
            peer = bias * side + lax.rem(place.seat + j, side)
            k = lax.rem(peer - me + n, n)

            @pl.when(k == 0)
            def _():
                own_incoming(s, q).start()

            @pl.when(k != 0)
            def _():
                incoming(s, q, k).start()

        loop(0, side, send_one)

    def mine(q):
        return pl.ds((q * n + member) * group, group)

    def polar(q, k):
        peer = lax.rem(member + k, n)
        return pltpu.make_async_remote_copy(
            src_ref=folded.at[:, pl.ds(q * group, group), pl.ds(peer * each, each)],
            dst_ref=mixed.at[:, mine(q)],
            send_sem=p_send.at[q],
            recv_sem=p_recv.at[q],
            device_id=place.of_member(peer),
            device_id_type=MESH,
        )

    def own_polar(q):
        return pltpu.make_async_copy(
            folded.at[:, pl.ds(q * group, group), pl.ds(member * each, each)],
            mixed.at[:, mine(q)],
            p_recv.at[q],
        )

    def screened(q, k):
        peer = lax.rem(member + k, n)
        return pltpu.make_async_remote_copy(
            src_ref=screen.at[:, pl.ds((q * n + peer) * group, group)],
            dst_ref=other_buf.at[:, pl.ds(q * group, group), pl.ds(member * each, each)],
            send_sem=w_send.at[q],
            recv_sem=w_recv.at[q],
            device_id=place.of_member(peer),
            device_id_type=MESH,
        )

    def own_screened(q):
        return pltpu.make_async_copy(
            screen.at[:, mine(q)],
            other_buf.at[:, pl.ds(q * group, group), pl.ds(member * each, each)],
            w_recv.at[q],
        )

    def dressed(q, k):
        peer = lax.rem(me + k, n)
        return pltpu.make_async_remote_copy(
            src_ref=folded.at[:, pl.ds(q * group, group), pl.ds(peer * each, each)],
            dst_ref=sigma.at[:, mine(q)],
            send_sem=s_send.at[q],
            recv_sem=s_recv.at[q],
            device_id={"bias": half, "ea": peer},
            device_id_type=MESH,
        )

    def own_dressed(q):
        return pltpu.make_async_copy(
            folded.at[:, pl.ds(q * group, group), pl.ds(me * each, each)],
            sigma.at[:, mine(q)],
            s_recv.at[q],
        )

    def await_all(ref, sem):
        pltpu.make_async_copy(ref, ref, sem).wait()

    def chunk(ref, q):
        return ref.at[:, pl.ds(q * group, group)]

    def sent(ref, q, pieces):
        return ref.at[:, pl.ds(q * group, group), pl.ds(0, pieces * each)]

    raw = (
        pltpu.make_async_copy(lesser, lesser_raw, keep.at[0]),
        pltpu.make_async_copy(other, other_raw, keep.at[1]),
    )
    for copy in raw:
        copy.start()
    greet(place)
    raw[0].wait()

    def chunk_rows(q):
        return pl.ds(pl.multiple_of(q * 2 * wide, 2 * wide), 2 * wide)

    def regroup(q):
        for c in range(2):
            turned = jnp.swapaxes(lesser_raw[:, c, chunk_rows(q), :], 0, 1)
            for h in range(2):
                slot = jnp.where(plane == h, h, 2)
                lesser_rows[slot, c, pl.ds(q * wide, wide)] = turned[h * wide : (h + 1) * wide]
        swap(0, q).start()

    def turn(low, c):
        turned = jnp.stack([other_raw[e, c, :, low : low + LANES].T for e in range(each)], axis=0)
        turned = jnp.swapaxes(turned, 0, 1)
        for at in range(0, LANES, wide):
            piece = (low + at) // wide
            slot = jnp.where(plane == piece % 2, piece % 2, 2)
            start = piece // 2 * wide
            other_rows[slot, c, start : start + wide] = turned[at : at + wide]

    def relay(s, q):
        swap(s, q).wait_recv()
        spread(s, q, 1 - plane)

    def advance(q):
        for s in range(2):
            spread(s, q, plane)
            relay(s, q)

    def own_first(q):
        regroup(q)
        spread(0, q, plane)

    def both(q):
        regroup(q)
        swap(1, q).start()

    per = LANES // (2 * wide)
    loop(0, AHEAD, own_first)
    relay(0, 0)
    raw[1].wait()
    turn(0, 0)
    loop(1, AHEAD // 2 + 1, lambda q: relay(0, q))
    turn(0, 1)
    loop(0, AHEAD, lambda q: swap(1, q).start())
    spread(1, 0, plane)
    spread(1, 1, plane)
    loop(AHEAD // 2 + 1, AHEAD, lambda q: relay(0, q))
    loop(AHEAD, per, both)
    relay(1, 0)
    lows = [(low, c) for low in range(LANES, rows * n, LANES) for c in range(2)]
    for low, c in lows[: len(lows) // 2]:
        turn(low, c)
    relay(1, 1)
    spread(1, 2, plane)
    for low, c in lows[len(lows) // 2 :]:
        turn(low, c)
    relay(1, 2)

    def rest(q):
        spread(1, q, plane)
        relay(1, q)

    loop(3, AHEAD, rest)

    def absorb(q):
        await_all(mixed.at[:, chunk_rows(q)], p_recv.at[q])
        for c in range(2):
            lesser_raw[:, c, chunk_rows(q), :] = jnp.swapaxes(mixed[c, chunk_rows(q)], 0, 1)

    def work(q):
        @pl.when(q + per < CHUNKS)
        def _():
            both(q + per)

        @pl.when(q + AHEAD < CHUNKS)
        def _():
            advance(q + AHEAD)

        for s in range(2):
            await_all(chunk(targets[s], q), in_recv.at[s, q])
        loop(
            q * group,
            (q + 1) * group,
            functools.partial(
                fold_row, True, scale, count, table, table_t, lesser_buf, other_buf, folded, volts
            ),
        )
        loop(1, n, lambda k: polar(q, k).start())
        own_polar(q).start()

        @pl.when(q >= BEHIND)
        def _():
            absorb(q - BEHIND)

    loop(0, CHUNKS, work)
    loop(CHUNKS - BEHIND, CHUNKS, absorb)
    bare = volts[...]
    width = bare.shape[0]

    def screen_one(e):
        pair = lesser_raw[e].reshape(2 * width, width)
        by_real = dot(pair, lesser_raw[e, 0])
        by_imag = dot(pair, lesser_raw[e, 1])
        square_real = by_real[:width] - by_imag[width:]
        square_imag = by_imag[:width] + by_real[width:]
        inner = jnp.concatenate(
            [
                (lesser_raw[e, 0].astype(jnp.float32) + square_real).astype(jnp.bfloat16),
                (lesser_raw[e, 1].astype(jnp.float32) + square_imag).astype(jnp.bfloat16),
            ],
            axis=1,
        )
        result = dot(bare, inner)
        lesser_raw[e, 0] = (bare.astype(jnp.float32) + result[:, :width]).astype(jnp.bfloat16)
        lesser_raw[e, 1] = result[:, width:].astype(jnp.bfloat16)

    def screen_some(i):
        for j in range(UNROLL):
            screen_one(i * UNROLL + j)

    loop(0, each // UNROLL, screen_some)

    def send_screen(q):
        for c in range(2):
            screen[c, chunk_rows(q)] = jnp.swapaxes(lesser_raw[:, c, chunk_rows(q), :], 0, 1)
        loop(1, n, lambda k: screened(q, k).start())
        own_screened(q).start()

    loop(0, CHUNKS, send_screen)

    def settle(q):
        for s in range(2):
            swap(s, q).wait_send()
            await_all(sent(targets[s], q, n - 1), in_send.at[s, q])
        await_all(sent(folded, q, n - 1), p_send.at[q])

    loop(0, CHUNKS, settle)

    def dress(q):
        await_all(chunk(other_buf, q), w_recv.at[q])
        loop(
            q * group,
            (q + 1) * group,
            functools.partial(
                fold_row, False, scale, count, table, table_t, lesser_buf, other_buf, folded, None
            ),
        )

        def send_to(target_half):
            def send_one(j):
                peer = target_half * side + lax.rem(place.seat + j, side)
                dressed(q, lax.rem(peer - me + n, n)).start()

            return send_one

        loop(0, side, send_to(1 - half))

        @pl.when(at_home)
        def _():
            own_dressed(q).start()

        @pl.when(jnp.logical_not(at_home))
        def _():
            dressed(q, 0).start()

        loop(1, side, send_to(half))

    loop(0, CHUNKS, dress)

    def collect(q):
        await_all(sigma.at[:, chunk_rows(q)], s_recv.at[q])
        for c in range(2):
            lesser_raw[:, c, chunk_rows(q), :] = jnp.swapaxes(sigma[c, chunk_rows(q)], 0, 1)

    loop(0, CHUNKS, collect)
    result = pltpu.make_async_copy(lesser_raw, out, keep.at[0])
    result.start()

    def finish(q):
        await_all(sent(other_buf, q, n - 1), w_send.at[q])

        @pl.when(at_home)
        def _():
            await_all(sent(folded, q, n - 1), s_send.at[q])

        @pl.when(jnp.logical_not(at_home))
        def _():
            await_all(sent(folded, q, n), s_send.at[q])

    loop(0, CHUNKS, finish)
    result.wait()


def iterate(n, count, scale, g_lesser, g_greater, table, table_t, coulomb):
    each, _, orbitals, width = g_lesser.shape
    rows = orbitals // n
    hbm = pl.BlockSpec(memory_space=pl.ANY)
    vmem = pl.BlockSpec(memory_space=pltpu.VMEM)
    by_row = pltpu.VMEM((2, rows, count, width), jnp.bfloat16)
    by_energy = pltpu.VMEM((each, 2, orbitals, width), jnp.bfloat16)
    stage = pltpu.VMEM((3, 2, orbitals // 2, each, width), jnp.bfloat16)
    landing = pltpu.VMEM((2, orbitals, each, width), jnp.bfloat16)
    dma = pltpu.SemaphoreType.DMA
    return pl.pallas_call(
        functools.partial(gw_kernel, n, count, scale),
        name="iterate",
        out_shape=jax.ShapeDtypeStruct(g_lesser.shape, jnp.bfloat16),
        in_specs=[hbm, hbm, vmem, vmem, vmem],
        out_specs=hbm,
        scratch_shapes=[
            by_row, by_row, by_row, by_energy, by_energy, stage, stage,
            landing, landing, landing,
            dma((2, CHUNKS)), dma((2, CHUNKS)), dma((2, CHUNKS)), dma((2, CHUNKS)),
            dma((CHUNKS,)), dma((CHUNKS,)), dma((CHUNKS,)), dma((CHUNKS,)),
            dma((CHUNKS,)), dma((CHUNKS,)), dma((2,)),
        ],
        compiler_params=pltpu.CompilerParams(
            collective_id=0, has_side_effects=True, vmem_limit_bytes=VMEM_BYTES
        ),
    )(g_lesser, g_greater, table, table_t, coulomb)


def dot(left, right):
    return jnp.dot(left, right, preferred_element_type=jnp.float32)


def dyson_kernel(sigma, free, out):
    for e in range(sigma.shape[0]):
        real, imag = sigma[e, 0], sigma[e, 1]
        free_real, free_imag = free[e, 0], free[e, 1]
        right_real = (dot(real, free_real) - dot(imag, free_imag)).astype(jnp.bfloat16)
        right_imag = (dot(real, free_imag) + dot(imag, free_real)).astype(jnp.bfloat16)
        out_real = dot(free_real, right_real) - dot(free_imag, right_imag)
        out_imag = dot(free_real, right_imag) + dot(free_imag, right_real)
        out[e, 0] = (free_real.astype(jnp.float32) + out_real).astype(jnp.bfloat16)
        out[e, 1] = (free_imag.astype(jnp.float32) + out_imag).astype(jnp.bfloat16)


def per_energy(kernel, name, matrices, others):
    each, two, rows, width = matrices.shape
    block = pl.BlockSpec((2, two, rows, width), lambda i: (i, 0, 0, 0))
    specs = [block if other.ndim == 4 else pl.BlockSpec(memory_space=pltpu.VMEM) for other in others]
    products = 6 if name == "screen" else 8
    return pl.pallas_call(
        kernel,
        name=name,
        grid=(each // 2,),
        out_shape=jax.ShapeDtypeStruct(matrices.shape, jnp.bfloat16),
        in_specs=[block] + specs,
        out_specs=block,
        cost_estimate=pl.CostEstimate(
            flops=2 * products * each * rows * rows * width,
            bytes_accessed=4 * two * each * rows * width,
            transcendentals=0,
        ),
    )(matrices, *others)


def per_device(n, biases, g_lesser, g_greater, g_free, coulomb):
    each, _, orbitals, _ = g_lesser.shape
    count = n * each
    if biases != 2 or n % 2 or each % 16 or orbitals % (n * CHUNKS) or LANES % (orbitals // CHUNKS):
        return plain(g_lesser, g_greater, g_free, coulomb)
    scale = 1.0 / (2 * count * count)
    full = transform_table(count)
    table = jnp.asarray(full).astype(jnp.bfloat16)
    table_t = jnp.asarray(full.T).astype(jnp.bfloat16)
    sigma = iterate(n, count, scale, g_lesser, g_greater, table, table_t, coulomb)
    return per_energy(dyson_kernel, "dyson", sigma, (g_free,))


def solution(mesh):
    return jax.shard_map(
        functools.partial(per_device, mesh.shape["ea"], mesh.shape["bias"]),
        mesh=mesh,
        in_specs=(
            P(("bias", "ea"), None, None, None),
            P(("bias", "ea"), None, None, None),
            P(("bias", "ea"), None, None, None),
            P(),
        ),
        out_specs=P(("bias", "ea"), None, None, None),
        check_vma=False,
    )
```

```python
import functools
import math

import jax
import jax.numpy as jnp
import numpy as np
from jax import lax
from jax.experimental import pallas as pl
from jax.experimental.pallas import tpu as pltpu
from jax.sharding import PartitionSpec as P

NE = 256


def dft_tables(length, count):
    freq = jnp.arange(length, dtype=jnp.int32)
    places = jnp.arange(count, dtype=jnp.int32)
    phase = freq[:, None] * places[None, :] % length
    angle = phase.astype(jnp.float32) * (2.0 * math.pi / length)
    cosine = jnp.cos(angle)
    sine = jnp.sin(angle)
    stacked = jnp.concatenate([cosine, sine], axis=0)
    upper = stacked.astype(jnp.bfloat16)
    lower = (stacked - upper.astype(jnp.float32)).astype(jnp.bfloat16)
    backward = jnp.concatenate([cosine.T, sine.T], axis=0)
    return (upper, lower, backward)


def forward(tables, block, sign):
    upper, lower = tables
    length = upper.shape[0] // 2
    real_part = block[:, 0].reshape(block.shape[0], -1)
    imag_part = block[:, 1].reshape(block.shape[0], -1)
    width = real_part.shape[1]
    joined = jnp.concatenate([real_part, imag_part], axis=1)
    result = jnp.dot(upper, joined, preferred_element_type=jnp.float32)
    result = result + jnp.dot(lower, joined, preferred_element_type=jnp.float32)
    cos_real = result[:length, :width]
    cos_imag = result[:length, width:]
    sin_real = result[length:, :width]
    sin_imag = result[length:, width:]
    return (cos_real - sign * sin_imag, cos_imag + sign * sin_real)


def inverse(backward, real_part, imag_part, scale):
    count = backward.shape[0] // 2
    width = real_part.shape[1]
    joined = jnp.concatenate([real_part, imag_part], axis=1)
    result = jnp.dot(
        backward, joined, precision=lax.Precision.HIGH, preferred_element_type=jnp.float32
    )
    cos_real = result[:count, :width]
    cos_imag = result[:count, width:]
    sin_real = result[count:, :width]
    sin_imag = result[count:, width:]
    return ((cos_real - sin_imag) * scale, (cos_imag + sin_real) * scale)


def complex_mul(left, right):
    return (left[0] * right[0] - left[1] * right[1], left[0] * right[1] + left[1] * right[0])


def restack(real_part, imag_part, shape):
    return jnp.stack([real_part.reshape(shape), imag_part.reshape(shape)], axis=1).astype(
        jnp.bfloat16
    )


def batched(left, right):
    return jnp.einsum("eij,ejk->eik", left, right, preferred_element_type=jnp.float32)


def dyson(sigma_real, sigma_imag, g_free):
    free_real = g_free[:, 0]
    free_imag = g_free[:, 1]
    right_real = (batched(sigma_real, free_real) - batched(sigma_imag, free_imag)).astype(
        jnp.bfloat16
    )
    right_imag = (batched(sigma_real, free_imag) + batched(sigma_imag, free_real)).astype(
        jnp.bfloat16
    )
    out_real = (
        free_real.astype(jnp.float32)
        + batched(free_real, right_real)
        - batched(free_imag, right_imag)
    )
    out_imag = (
        free_imag.astype(jnp.float32)
        + batched(free_real, right_imag)
        + batched(free_imag, right_real)
    )
    return jnp.stack([out_real, out_imag], axis=1).astype(jnp.bfloat16)


def plain(g_lesser, g_greater, g_free, coulomb):
    length = 2 * NE
    upper, lower, backward = dft_tables(length, NE)
    tables = (upper, lower)
    scale = 1.0 / (length * NE)
    greater_t = jnp.swapaxes(g_greater, 2, 3)
    lesser_rows, greater_rows = (
        lax.all_to_all(g_lesser, "ea", split_axis=2, concat_axis=0, tiled=True),
        lax.all_to_all(greater_t, "ea", split_axis=2, concat_axis=0, tiled=True),
    )
    spec_lesser = forward(tables, lesser_rows, -1.0)
    element_shape = (NE, lesser_rows.shape[2], lesser_rows.shape[3])
    spec_greater = forward(tables, greater_rows, 1.0)
    joined = complex_mul(spec_lesser, spec_greater)
    polar_real, polar_imag = inverse(backward, joined[0], joined[1], scale)
    polar_rows = restack(polar_real, polar_imag, element_shape)
    polar = lax.all_to_all(polar_rows, "ea", split_axis=0, concat_axis=2, tiled=True)
    mixed_real = jnp.einsum(
        "eij,jk->eik", polar[:, 0], coulomb, preferred_element_type=jnp.float32
    ).astype(jnp.bfloat16)
    mixed_imag = jnp.einsum(
        "eij,jk->eik", polar[:, 1], coulomb, preferred_element_type=jnp.float32
    ).astype(jnp.bfloat16)
    square_real = batched(mixed_real, mixed_real) - batched(mixed_imag, mixed_imag)
    square_imag = batched(mixed_real, mixed_imag) + batched(mixed_imag, mixed_real)
    inner_real = (mixed_real.astype(jnp.float32) + square_real).astype(jnp.bfloat16)
    inner_imag = (mixed_imag.astype(jnp.float32) + square_imag).astype(jnp.bfloat16)
    screen_real = coulomb.astype(jnp.float32)[None] + jnp.einsum(
        "ij,ejk->eik", coulomb, inner_real, preferred_element_type=jnp.float32
    )
    screen_imag = jnp.einsum("ij,ejk->eik", coulomb, inner_imag, preferred_element_type=jnp.float32)
    screen = jnp.stack([screen_real, screen_imag], axis=1).astype(jnp.bfloat16)
    screen_rows = lax.all_to_all(screen, "ea", split_axis=2, concat_axis=0, tiled=True)
    spec_screen = forward(tables, screen_rows, -1.0)
    folded = complex_mul(spec_lesser, spec_screen)
    sigma_real, sigma_imag = inverse(backward, folded[0], folded[1], scale)
    sigma_rows = restack(sigma_real, sigma_imag, element_shape)
    sigma = lax.all_to_all(sigma_rows, "ea", split_axis=0, concat_axis=2, tiled=True)
    return dyson(sigma[:, 0], sigma[:, 1], g_free)


MESH = pl.DeviceIdType.MESH
CHUNKS = 16
BLOCKS = 4
AHEAD = 6
BEHIND = 4
UNROLL = 4
LANES = 128
VMEM_BYTES = 60 * 1024 * 1024


def transform_table(count):
    length = 2 * count
    phase = np.arange(length)[:, None] * np.arange(count)[None, :] % length
    angle = phase * (2.0 * math.pi / length)
    cosine, sine = np.cos(angle), np.sin(angle)
    return np.block([[cosine, sine], [-sine, cosine]]).astype(np.float32)


class Place:
    def __init__(self, n):
        self.n = n
        self.side = n // 2
        self.plane = lax.axis_index("bias")
        self.me = lax.axis_index("ea")
        self.half = lax.div(self.me, self.side)
        self.seat = lax.rem(self.me, self.side)
        self.member = self.plane * self.side + self.seat

    def of_member(self, member):
        return {
            "bias": lax.div(member, self.side),
            "ea": self.half * self.side + lax.rem(member, self.side),
        }


def greet(place):
    n = place.n
    barrier = pltpu.get_barrier_semaphore()
    mine = place.plane * n + place.me

    def hello(k, carry):
        other = lax.rem(mine + k, 2 * n)
        pl.semaphore_signal(
            barrier,
            inc=1,
            device_id={"bias": lax.div(other, n), "ea": lax.rem(other, n)},
            device_id_type=MESH,
        )
        return carry

    lax.fori_loop(1, 2 * n, hello, 0)
    pl.semaphore_wait(barrier, 2 * n - 1)


def loop(low, high, body):
    def step(k, carry):
        body(k)
        return carry

    lax.fori_loop(low, high, step, 0)


def fold_row(first, scale, count, table, table_t, lesser_buf, other_buf, folded, volts, row):
    length = 2 * count
    left = jnp.concatenate([lesser_buf[0, row], lesser_buf[1, row]], axis=0)
    imag = other_buf[1, row]
    right = jnp.concatenate([other_buf[0, row], -imag if first else imag], axis=0)
    left_spec = jnp.dot(table[...], left, preferred_element_type=jnp.float32)
    right_spec = jnp.dot(table[...], right, preferred_element_type=jnp.float32)
    left_real, left_imag = left_spec[:length], left_spec[length:]
    right_real, right_imag = right_spec[:length], right_spec[length:]
    if first:
        real = left_real * right_real + left_imag * right_imag
        imag = left_imag * right_real - left_real * right_imag
    else:
        real = left_real * right_real - left_imag * right_imag
        imag = left_real * right_imag + left_imag * right_real
    product = jnp.concatenate([real, imag], axis=0).astype(jnp.bfloat16)
    result = jnp.dot(table_t[...], product, preferred_element_type=jnp.float32) * scale
    result = result.astype(jnp.bfloat16)
    if first:
        result = jnp.dot(result, volts[...], preferred_element_type=jnp.float32)
        result = result.astype(jnp.bfloat16)
    folded[0, row] = result[:count]
    folded[1, row] = result[count:]


def gw_kernel(
    n, count, scale, lesser, other, free, table, table_t, volts, out,
    lesser_buf, other_buf, folded, lesser_raw, other_raw, lesser_rows, other_rows,
    mixed, screen, sigma,
    in_send, in_recv, swap_send, swap_recv, p_send, p_recv, w_send, w_recv, s_send, s_recv, keep, finals,
):
    place = Place(n)
    me, plane, half, side = place.me, place.plane, place.half, place.side
    member = place.member
    rows = folded.shape[1]
    each = count // n
    group = rows // CHUNKS
    wide = side * group
    stages = (lesser_rows, other_rows)
    targets = (lesser_buf, other_buf)
    at_home = plane == half

    def swap(s, q):
        span = pl.ds(q * wide, wide)
        return pltpu.make_async_remote_copy(
            src_ref=stages[s].at[2, :, span],
            dst_ref=stages[s].at[plane, :, span],
            send_sem=swap_send.at[s, q],
            recv_sem=swap_recv.at[s, q],
            device_id={"bias": 1 - plane},
            device_id_type=MESH,
        )

    def ends(s, q, peer):
        source = stages[s].at[
            lax.div(peer, side), :, pl.ds(q * wide + lax.rem(peer, side) * group, group)
        ]
        target = targets[s].at[:, pl.ds(q * group, group), pl.ds(me * each, each)]
        return source, target

    def incoming(s, q, k):
        peer = lax.rem(me + k, n)
        source, target = ends(s, q, peer)
        return pltpu.make_async_remote_copy(
            src_ref=source,
            dst_ref=target,
            send_sem=in_send.at[s, q],
            recv_sem=in_recv.at[s, q],
            device_id={"ea": peer},
            device_id_type=MESH,
        )

    def own_incoming(s, q):
        source, target = ends(s, q, me)
        return pltpu.make_async_copy(source, target, in_recv.at[s, q])

    def spread(s, q, bias):
        def send_one(j):
            peer = bias * side + lax.rem(place.seat + j, side)
            k = lax.rem(peer - me + n, n)

            @pl.when(k == 0)
            def _():
                own_incoming(s, q).start()

            @pl.when(k != 0)
            def _():
                incoming(s, q, k).start()

        loop(0, side, send_one)

    def mine(q):
        return pl.ds((q * n + member) * group, group)

    def polar(q, k):
        peer = lax.rem(member + k, n)
        return pltpu.make_async_remote_copy(
            src_ref=folded.at[:, pl.ds(q * group, group), pl.ds(peer * each, each)],
            dst_ref=mixed.at[:, mine(q)],
            send_sem=p_send.at[q],
            recv_sem=p_recv.at[q],
            device_id=place.of_member(peer),
            device_id_type=MESH,
        )

    def own_polar(q):
        return pltpu.make_async_copy(
            folded.at[:, pl.ds(q * group, group), pl.ds(member * each, each)],
            mixed.at[:, mine(q)],
            p_recv.at[q],
        )

    def screened(q, k):
        peer = lax.rem(member + k, n)
        return pltpu.make_async_remote_copy(
            src_ref=screen.at[:, pl.ds((q * n + peer) * group, group)],
            dst_ref=other_buf.at[:, pl.ds(q * group, group), pl.ds(member * each, each)],
            send_sem=w_send.at[q],
            recv_sem=w_recv.at[q],
            device_id=place.of_member(peer),
            device_id_type=MESH,
        )

    def own_screened(q):
        return pltpu.make_async_copy(
            screen.at[:, mine(q)],
            other_buf.at[:, pl.ds(q * group, group), pl.ds(member * each, each)],
            w_recv.at[q],
        )

    def dressed(q, k):
        peer = lax.rem(me + k, n)
        return pltpu.make_async_remote_copy(
            src_ref=folded.at[:, pl.ds(q * group, group), pl.ds(peer * each, each)],
            dst_ref=sigma.at[:, mine(q)],
            send_sem=s_send.at[q],
            recv_sem=s_recv.at[q],
            device_id={"bias": half, "ea": peer},
            device_id_type=MESH,
        )

    def own_dressed(q):
        return pltpu.make_async_copy(
            folded.at[:, pl.ds(q * group, group), pl.ds(me * each, each)],
            sigma.at[:, mine(q)],
            s_recv.at[q],
        )

    def await_all(ref, sem):
        pltpu.make_async_copy(ref, ref, sem).wait()

    def chunk(ref, q):
        return ref.at[:, pl.ds(q * group, group)]

    def sent(ref, q, pieces):
        return ref.at[:, pl.ds(q * group, group), pl.ds(0, pieces * each)]

    raw = (
        pltpu.make_async_copy(lesser, lesser_raw, keep.at[0]),
        pltpu.make_async_copy(other, other_raw, keep.at[1]),
    )
    for copy in raw:
        copy.start()
    greet(place)
    raw[0].wait()

    def chunk_rows(q):
        return pl.ds(pl.multiple_of(q * 2 * wide, 2 * wide), 2 * wide)

    def regroup(q):
        for c in range(2):
            turned = jnp.swapaxes(lesser_raw[:, c, chunk_rows(q), :], 0, 1)
            for h in range(2):
                slot = jnp.where(plane == h, h, 2)
                lesser_rows[slot, c, pl.ds(q * wide, wide)] = turned[h * wide : (h + 1) * wide]
        swap(0, q).start()

    def turn(low, c):
        turned = jnp.stack([other_raw[e, c, :, low : low + LANES].T for e in range(each)], axis=0)
        turned = jnp.swapaxes(turned, 0, 1)
        for at in range(0, LANES, wide):
            piece = (low + at) // wide
            slot = jnp.where(plane == piece % 2, piece % 2, 2)
            start = piece // 2 * wide
            other_rows[slot, c, start : start + wide] = turned[at : at + wide]

    def relay(s, q):
        swap(s, q).wait_recv()
        spread(s, q, 1 - plane)

    def advance(q):
        for s in range(2):
            spread(s, q, plane)
            relay(s, q)

    def own_first(q):
        regroup(q)
        spread(0, q, plane)

    def both(q):
        regroup(q)
        swap(1, q).start()

    per = LANES // (2 * wide)
    loop(0, AHEAD, own_first)
    relay(0, 0)
    raw[1].wait()
    turn(0, 0)
    loop(1, AHEAD // 2 + 1, lambda q: relay(0, q))
    turn(0, 1)
    loop(0, AHEAD, lambda q: swap(1, q).start())
    spread(1, 0, plane)
    spread(1, 1, plane)
    loop(AHEAD // 2 + 1, AHEAD, lambda q: relay(0, q))
    loop(AHEAD, per, both)
    relay(1, 0)
    lows = [(low, c) for low in range(LANES, rows * n, LANES) for c in range(2)]
    for low, c in lows[: len(lows) // 2]:
        turn(low, c)
    relay(1, 1)
    spread(1, 2, plane)
    for low, c in lows[len(lows) // 2 :]:
        turn(low, c)
    relay(1, 2)

    def rest(q):
        spread(1, q, plane)
        relay(1, q)

    loop(3, AHEAD, rest)

    def absorb(q):
        await_all(mixed.at[:, chunk_rows(q)], p_recv.at[q])
        for c in range(2):
            lesser_raw[:, c, chunk_rows(q), :] = jnp.swapaxes(mixed[c, chunk_rows(q)], 0, 1)

    def work(q):
        @pl.when(q + per < CHUNKS)
        def _():
            both(q + per)

        @pl.when(q + AHEAD < CHUNKS)
        def _():
            advance(q + AHEAD)

        for s in range(2):
            await_all(chunk(targets[s], q), in_recv.at[s, q])
        loop(
            q * group,
            (q + 1) * group,
            functools.partial(
                fold_row, True, scale, count, table, table_t, lesser_buf, other_buf, folded, volts
            ),
        )
        loop(1, n, lambda k: polar(q, k).start())
        own_polar(q).start()

        @pl.when(q >= BEHIND)
        def _():
            absorb(q - BEHIND)

    loop(0, CHUNKS, work)
    loop(CHUNKS - BEHIND, CHUNKS, absorb)
    free_copy = pltpu.make_async_copy(free, other_raw, keep.at[1])
    free_copy.start()
    bare = volts[...]
    width = bare.shape[0]

    def screen_one(e):
        pair = lesser_raw[e].reshape(2 * width, width)
        by_real = dot(pair, lesser_raw[e, 0])
        by_imag = dot(pair, lesser_raw[e, 1])
        square_real = by_real[:width] - by_imag[width:]
        square_imag = by_imag[:width] + by_real[width:]
        inner = jnp.concatenate(
            [
                (lesser_raw[e, 0].astype(jnp.float32) + square_real).astype(jnp.bfloat16),
                (lesser_raw[e, 1].astype(jnp.float32) + square_imag).astype(jnp.bfloat16),
            ],
            axis=1,
        )
        result = dot(bare, inner)
        lesser_raw[e, 0] = (bare.astype(jnp.float32) + result[:, :width]).astype(jnp.bfloat16)
        lesser_raw[e, 1] = result[:, width:].astype(jnp.bfloat16)

    def screen_some(i):
        for j in range(UNROLL):
            screen_one(i * UNROLL + j)

    loop(0, each // UNROLL, screen_some)

    def send_screen(q):
        for c in range(2):
            screen[c, chunk_rows(q)] = jnp.swapaxes(lesser_raw[:, c, chunk_rows(q), :], 0, 1)
        loop(1, n, lambda k: screened(q, k).start())
        own_screened(q).start()

    loop(0, CHUNKS, send_screen)

    def settle(q):
        for s in range(2):
            swap(s, q).wait_send()
            await_all(sent(targets[s], q, n - 1), in_send.at[s, q])
        await_all(sent(folded, q, n - 1), p_send.at[q])

    loop(0, CHUNKS, settle)

    def dress(q):
        await_all(chunk(other_buf, q), w_recv.at[q])
        loop(
            q * group,
            (q + 1) * group,
            functools.partial(
                fold_row, False, scale, count, table, table_t, lesser_buf, other_buf, folded, None
            ),
        )

        def send_far(j):
            peer = (1 - half) * side + lax.rem(place.seat + j, side)
            dressed(q, lax.rem(peer - me + n, n)).start()

        loop(0, side, send_far)

    loop(0, CHUNKS, dress)

    def dress_near(q):
        @pl.when(at_home)
        def _():
            own_dressed(q).start()

        @pl.when(jnp.logical_not(at_home))
        def _():
            dressed(q, 0).start()

        def send_near(j):
            peer = half * side + lax.rem(place.seat + j, side)
            dressed(q, lax.rem(peer - me + n, n)).start()

        loop(1, side, send_near)

    loop(0, CHUNKS, dress_near)

    def collect(q):
        await_all(sigma.at[:, chunk_rows(q)], s_recv.at[q])
        for c in range(2):
            lesser_raw[:, c, chunk_rows(q), :] = jnp.swapaxes(sigma[c, chunk_rows(q)], 0, 1)

    span = width // BLOCKS

    def result(i):
        block = pl.ds(pl.multiple_of(i * span, span), span)
        return pltpu.make_async_copy(
            lesser_raw.at[:, :, block], out.at[:, :, block], finals.at[i]
        )

    def correct(i):
        loop(i * (CHUNKS // BLOCKS), (i + 1) * (CHUNKS // BLOCKS), collect)
        block = pl.ds(pl.multiple_of(i * span, span), span)

        def correct_some(j):
            for e in range(UNROLL):
                e = j * UNROLL + e
                pair = jnp.concatenate([lesser_raw[e, 0, block], lesser_raw[e, 1, block]], axis=0)
                by_real = dot(pair, other_raw[e, 0])
                by_imag = dot(pair, other_raw[e, 1])
                lesser_raw[e, 0, block] = (by_real[:span] - by_imag[span:]).astype(jnp.bfloat16)
                lesser_raw[e, 1, block] = (by_imag[:span] + by_real[span:]).astype(jnp.bfloat16)

        loop(0, each // UNROLL, correct_some)
        result(i).start()

    free_copy.wait()
    loop(0, BLOCKS, correct)

    def finish(q):
        await_all(sent(other_buf, q, n - 1), w_send.at[q])

        @pl.when(at_home)
        def _():
            await_all(sent(folded, q, n - 1), s_send.at[q])

        @pl.when(jnp.logical_not(at_home))
        def _():
            await_all(sent(folded, q, n), s_send.at[q])

    loop(0, CHUNKS, finish)
    loop(0, BLOCKS, lambda i: result(i).wait())


def iterate(n, count, scale, g_lesser, g_greater, g_free, table, table_t, coulomb):
    each, _, orbitals, width = g_lesser.shape
    rows = orbitals // n
    hbm = pl.BlockSpec(memory_space=pl.ANY)
    vmem = pl.BlockSpec(memory_space=pltpu.VMEM)
    by_row = pltpu.VMEM((2, rows, count, width), jnp.bfloat16)
    by_energy = pltpu.VMEM((each, 2, orbitals, width), jnp.bfloat16)
    stage = pltpu.VMEM((3, 2, orbitals // 2, each, width), jnp.bfloat16)
    landing = pltpu.VMEM((2, orbitals, each, width), jnp.bfloat16)
    dma = pltpu.SemaphoreType.DMA
    return pl.pallas_call(
        functools.partial(gw_kernel, n, count, scale),
        name="iterate",
        out_shape=jax.ShapeDtypeStruct(g_lesser.shape, jnp.bfloat16),
        in_specs=[hbm, hbm, hbm, vmem, vmem, vmem],
        out_specs=hbm,
        scratch_shapes=[
            by_row, by_row, by_row, by_energy, by_energy, stage, stage,
            landing, landing, landing,
            dma((2, CHUNKS)), dma((2, CHUNKS)), dma((2, CHUNKS)), dma((2, CHUNKS)),
            dma((CHUNKS,)), dma((CHUNKS,)), dma((CHUNKS,)), dma((CHUNKS,)),
            dma((CHUNKS,)), dma((CHUNKS,)), dma((2,)), dma((BLOCKS,)),
        ],
        compiler_params=pltpu.CompilerParams(
            collective_id=0, has_side_effects=True, vmem_limit_bytes=VMEM_BYTES
        ),
    )(g_lesser, g_greater, g_free, table, table_t, coulomb)


def dot(left, right):
    return jnp.dot(left, right, preferred_element_type=jnp.float32)


def dyson_kernel(right, free, out):
    rows = right.shape[2]
    for e in range(right.shape[0]):
        pair = free[e].reshape(2 * rows, rows)
        by_real = dot(pair, right[e, 0])
        by_imag = dot(pair, right[e, 1])
        out_real = by_real[:rows] - by_imag[rows:]
        out_imag = by_imag[:rows] + by_real[rows:]
        out[e, 0] = (free[e, 0].astype(jnp.float32) + out_real).astype(jnp.bfloat16)
        out[e, 1] = (free[e, 1].astype(jnp.float32) + out_imag).astype(jnp.bfloat16)


def per_energy(kernel, name, matrices, others):
    each, two, rows, width = matrices.shape
    block = pl.BlockSpec((4, two, rows, width), lambda i: (i, 0, 0, 0))
    specs = [block if other.ndim == 4 else pl.BlockSpec(memory_space=pltpu.VMEM) for other in others]
    products = 4
    return pl.pallas_call(
        kernel,
        name=name,
        grid=(each // 4,),
        out_shape=jax.ShapeDtypeStruct(matrices.shape, jnp.bfloat16),
        in_specs=[block] + specs,
        out_specs=block,
        cost_estimate=pl.CostEstimate(
            flops=2 * products * each * rows * rows * width,
            bytes_accessed=4 * two * each * rows * width,
            transcendentals=0,
        ),
    )(matrices, *others)


def per_device(n, biases, g_lesser, g_greater, g_free, coulomb):
    each, _, orbitals, _ = g_lesser.shape
    count = n * each
    if biases != 2 or n % 2 or each % 16 or orbitals % (n * CHUNKS) or LANES % (orbitals // CHUNKS):
        return plain(g_lesser, g_greater, g_free, coulomb)
    scale = 1.0 / (2 * count * count)
    full = transform_table(count)
    table = jnp.asarray(full).astype(jnp.bfloat16)
    table_t = jnp.asarray(full.T).astype(jnp.bfloat16)
    right = iterate(n, count, scale, g_lesser, g_greater, g_free, table, table_t, coulomb)
    return per_energy(dyson_kernel, "dyson", right, (g_free,))


def solution(mesh):
    return jax.shard_map(
        functools.partial(per_device, mesh.shape["ea"], mesh.shape["bias"]),
        mesh=mesh,
        in_specs=(
            P(("bias", "ea"), None, None, None),
            P(("bias", "ea"), None, None, None),
            P(("bias", "ea"), None, None, None),
            P(),
        ),
        out_specs=P(("bias", "ea"), None, None, None),
        check_vma=False,
    )
```
